32 devices in a mesh: frame: 8 (over z, x), row: 4 (over y, core).
Axes of the slice: x: 2, y: 2, z: 4, core: 2. Of those that a mesh axis runs over, the one named last changes fastest.
Arguments:
- clip: bfloat16 [16, 16, 256, 128], P('frame', 'row'), may hold values from -6 to 6
- first_kernel: bfloat16 [3, 3, 3, 128, 128], replicated, may hold values from -0.109375 to 0.109375
- second_kernel: bfloat16 [3, 3, 3, 128, 128], replicated, may hold values from -0.109375 to 0.109375
- cotangent: bfloat16 [16, 16, 256, 128], P('frame', 'row'), may hold values from -6 to 6
Outputs:
- critic_map: bfloat16 [16, 16, 256, 128], P('frame', 'row')
- clip_grad: bfloat16 [16, 16, 256, 128], P('frame', 'row')
- first_grad: float32 [3, 3, 3, 128, 128], replicated
- second_grad: float32 [3, 3, 3, 128, 128], replicated
The draws below stay inside these ranges and needn't reach their ends.
All inputs are finite; a program needn't handle non-finite values.
Results may differ from the reference program's by a relative error of at most 0.012.
Values may be sent and summed in bfloat16 or wider, within the bound.
A program may use at most 64 MiB of HBM per device.

```python
import jax
import jax.numpy as jnp
from jax import lax

CH = 128
WIDTH = 256
FRAMES = 16
ROWS = 16


def level_of(stream_key, extent, shards, low, high):
    loudness = 1.0
    for position, parts in shards:
        draws = jax.random.uniform(jax.random.fold_in(jax.random.fold_in(stream_key, 6), position), (parts,), jnp.float32, low / len(shards), high / len(shards))
        loudness = loudness * jnp.repeat(jnp.exp(draws), extent[position] // parts).reshape((-1,) + (1,) * (len(extent) - 1 - position))
    return loudness


def centred(rng, extent, scale, most, cuts=(), held_as=jnp.bfloat16):
    gain = level_of(rng, extent, cuts, -0.22, 0.18) if cuts else 1.0
    values = jax.random.normal(rng, extent, jnp.float32) * scale * gain
    return jnp.minimum(jnp.maximum(values, -most), most).astype(held_as)


def setup_inputs(seed: int = 0) -> dict:
    key_list = jax.random.split(jax.random.key(seed), 5)
    clip = centred(key_list[0], (FRAMES, ROWS, WIDTH, CH), 1.0, 6.0, ((0, 8), (1, 4)))
    first_kernel = centred(key_list[1], (3, 3, 3, CH, CH), (27 * CH) ** -0.5, 0.109375)
    second_kernel = centred(key_list[2], (3, 3, 3, CH, CH), (27 * CH) ** -0.5, 0.109375)
    cotangent = centred(key_list[3], (FRAMES, ROWS, WIDTH, CH), 1.0, 6.0, ((0, 8), (1, 4)))
    return dict(clip=clip, first_kernel=first_kernel, second_kernel=second_kernel, cotangent=cotangent)


def correlate(padded, kernel):
    result = lax.conv_general_dilated(padded[None], kernel, (1, 1, 1), ((0, 0), (0, 0), (1, 1)), dimension_numbers=('NDHWC', 'DHWIO', 'NDHWC'), preferred_element_type=jnp.float32)
    return result[0]

def silu_slope(value):
    sigma = jax.nn.sigmoid(value)
    return sigma * (1.0 + value * (1.0 - sigma))

def flipped_kernel(kernel):
    return jnp.transpose(kernel[::-1, ::-1, ::-1], (0, 1, 2, 4, 3))

def weight_grad(padded, delta):
    frame_count, row_count, columns, channels = delta.shape
    widened = jnp.pad(padded, ((0, 0), (0, 0), (1, 1), (0, 0)))
    flat_delta = delta.reshape(-1, channels)
    blocks = []
    for frame_off in range(3):
        for row_off in range(3):
            for col_off in range(3):
                window_slab = widened[frame_off:frame_off + frame_count, row_off:row_off + row_count, col_off:col_off + columns]
                blocks.append(lax.dot_general(window_slab.reshape(-1, channels), flat_delta, (((0,), (0,)), ((), ())), preferred_element_type=jnp.float32))
    return jnp.stack(blocks).reshape(3, 3, 3, channels, channels)

def reference(clip, first_kernel, second_kernel, cotangent):
    grad_scale = 1.0 / float(FRAMES * ROWS * WIDTH) ** 0.5
    clip_pad = jnp.pad(clip, ((2, 0), (1, 1), (0, 0), (0, 0)))
    first_pre = correlate(clip_pad, first_kernel)
    first_act = jax.nn.silu(first_pre).astype(jnp.bfloat16)
    act_pad = jnp.pad(first_act, ((2, 0), (1, 1), (0, 0), (0, 0)))
    second_pre = correlate(act_pad, second_kernel)
    critic_map = jax.nn.silu(second_pre).astype(jnp.bfloat16)
    second_delta = (cotangent.astype(jnp.float32) * silu_slope(second_pre)).astype(jnp.bfloat16)
    second_grad = weight_grad(act_pad, second_delta) * grad_scale
    first_back = correlate(jnp.pad(second_delta, ((0, 2), (1, 1), (0, 0), (0, 0))), flipped_kernel(second_kernel))
    first_delta = (first_back * silu_slope(first_pre)).astype(jnp.bfloat16)
    first_grad = weight_grad(clip_pad, first_delta) * grad_scale
    clip_grad = correlate(jnp.pad(first_delta, ((0, 2), (1, 1), (0, 0), (0, 0))), flipped_kernel(first_kernel)).astype(jnp.bfloat16)
    return (critic_map, clip_grad, first_grad, second_grad)
```

```python
import functools

import jax
import jax.numpy as jnp
from jax import lax
from jax.experimental import pallas as pl
from jax.experimental.pallas import tpu as pltpu
from jax.sharding import PartitionSpec as P

MESH = pl.DeviceIdType.MESH
BF16, F32 = jnp.bfloat16, jnp.float32
MARGIN = 8
HALO = 2


def sum_groups(n_frame, n_row, me_f, me_r):
    pair, member = me_f // 2, lax.rem(me_f, 2)
    side, core = me_r // 2, lax.rem(me_r, 2)
    return (
        (2, core, lambda j: {"row": side * 2 + j}),
        (n_row // 2 * 2, side * 2 + member, lambda j: {"row": j // 2 * 2 + core, "frame": pair * 2 + lax.rem(j, 2)}),
        (n_frame // 2, pair, lambda j: {"frame": j * 2 + member}),
    )


def kernel(
    n_frame, n_row, grad_scale,
    clip, w1, w2, cot,
    critic, clip_grad, total1, total2,
    pads, cross, cotp, crit_s, cg_s, slope1, w1v, w2v, w1t, w2t, xt, d3, acc,
    mine, land_a, sum_a, land_b, sum_b, land_c,
    l_sem, x_send, x_recv, o_send, o_recv, f_send, f_recv, r_send, r_recv, s_send, s_recv, t_send, t_recv,
):
    step, rows, width, ch = clip.shape
    half = width // 2
    cw = half + MARGIN
    frames = 2 * step
    me_f, me_r = lax.axis_index("frame"), lax.axis_index("row")
    member = lax.rem(me_f, 2)
    first, second = member == 0, member == 1
    later, earlier = me_f < n_frame - 2, me_f > 1
    below, above = me_r < n_row - 1, me_r > 0
    partner = {"frame": me_f + 1 - 2 * member}
    groups = sum_groups(n_frame, n_row, me_f, me_r)
    own = pl.multiple_of(member * MARGIN, MARGIN)

    def start_of(who):
        return pl.multiple_of(who * (half - MARGIN), MARGIN)

    barrier = pltpu.get_barrier_semaphore()
    for there, who in ((below, {"row": me_r + 1}), (above, {"row": me_r - 1})):
        @pl.when(there)
        def _():
            pl.semaphore_signal(barrier, inc=1, device_id=who, device_id_type=MESH)
    greeted = below.astype(jnp.int32) + above.astype(jnp.int32)
    for count, index, device in groups[1:]:
        for d in range(1, count):
            pl.semaphore_signal(barrier, inc=1, device_id=device(lax.rem(index + d, count)), device_id_type=MESH)
        greeted = greeted + (count - 1)

    loads = []
    for t in range(step):
        mine_at, other_at = pl.ds(start_of(member), cw), pl.ds(start_of(1 - member), cw)
        loads.append((clip.at[t, :, other_at], cross.at[t]))
        loads.append((clip.at[t, :, mine_at], pads.at[0, HALO + step * member + t, pl.ds(1, rows)]))
    loads.append((w1, w1v))
    loads.append((w2, w2v))
    for t in range(step):
        loads.append((cot.at[t, :, mine_at], cotp.at[step * member + t]))
    loads = [pltpu.make_async_copy(a, b, l_sem.at[i]) for i, (a, b) in enumerate(loads)]
    for load in loads:
        load.start()

    def zero(ref):
        ref[...] = jnp.zeros(ref.shape, ref.dtype)

    for k in range(4):
        @pl.when(jnp.logical_not(earlier if k < 2 else later))
        def _():
            for f in ((0, 1) if k < 2 else (frames, frames + 1)):
                zero(pads.at[k, f])

        @pl.when(jnp.logical_not(above))
        def _():
            for f in range(frames + HALO):
                zero(pads.at[k, f, 0])

        @pl.when(jnp.logical_not(below))
        def _():
            for f in range(frames + HALO):
                zero(pads.at[k, f, rows + 1])
    used = 27 * ch
    for i in range(2):
        mine[i, pl.ds(used, mine.shape[1] - used)] = jnp.zeros((mine.shape[1] - used, ch), BF16)

    pl.semaphore_wait(barrier, greeted)

    def remote(src, dst, send, recv, who):
        return pltpu.make_async_remote_copy(
            src_ref=src, dst_ref=dst, send_sem=send, recv_sem=recv, device_id=who, device_id_type=MESH
        )

    def cross_copy(i, t):
        if i == 0:
            src, dst = cross.at[t], pads.at[0, HALO + step * member + t, pl.ds(1, rows)]
        else:
            src, dst = cot.at[t, :, pl.ds(start_of(1 - member), cw)], cotp.at[step * member + t]
        return remote(src, dst, x_send.at[i, t], x_recv.at[i, t], partner)

    def out_copy(i, t):
        src, dst = ((crit_s, critic), (cg_s, clip_grad))[i]
        return remote(
            src.at[step * (1 - member) + t, :, pl.ds(own, half)],
            dst.at[t, :, pl.ds(pl.multiple_of(member * half, half), half)],
            o_send.at[i, t], o_recv.at[i, t], partner,
        )

    def keep_copy(i, t):
        src, dst = ((crit_s, critic), (cg_s, clip_grad))[i]
        return pltpu.make_async_copy(
            src.at[step * member + t, :, pl.ds(own, half)],
            dst.at[t, :, pl.ds(pl.multiple_of(member * half, half), half)],
            l_sem.at[i * step + t],
        )

    def frame_copy(k, t):
        fwd = k < 2
        src, dst = (frames + t, t) if fwd else (t, frames + t)
        return remote(
            pads.at[k, src, pl.ds(1, rows)], pads.at[k, dst, pl.ds(1, rows)],
            f_send.at[k, t], f_recv.at[k, t], {"frame": me_f + 2 if fwd else me_f - 2},
        )

    def row_copy(k, f, way):
        src, dst = ((rows, 0), (1, rows + 1))[way]
        return remote(
            pads.at[k, f, src], pads.at[k, f, dst],
            r_send.at[k, f, way], r_recv.at[k, f, way], {"row": me_r + 1 if way == 0 else me_r - 1},
        )

    def send_rows(k, f):
        @pl.when(below)
        def _():
            row_copy(k, f, 0).start()

        @pl.when(above)
        def _():
            row_copy(k, f, 1).start()

    def wait_rows(k, fs):
        for f in fs:
            @pl.when(above)
            def _():
                row_copy(k, f, 0).wait_recv()

            @pl.when(below)
            def _():
                row_copy(k, f, 1).wait_recv()

    def send_frame(k, t):
        @pl.when(later if k < 2 else earlier)
        def _():
            frame_copy(k, t).start()

    def take_halo(k):
        fwd = k < 2

        @pl.when(earlier if fwd else later)
        def _():
            for t in ((1, 0) if fwd else (0, 1)):
                frame_copy(k, t).wait_recv()
                send_rows(k, t if fwd else frames + t)
            wait_rows(k, (1, 0) if fwd else (frames, frames + 1))

    def spans():
        lo, size, out = 0, mine.shape[1], []
        for count, index, _ in groups:
            size //= count
            lo = lo + index * size
            out.append((lo, size))
        return out

    parts = spans()

    def scatter_copy(i, level, d):
        count, index, device = groups[level]
        size = parts[level][1]
        src = (mine.at[i], sum_a.at[i], sum_b.at[i])[level]
        peer = lax.rem(index + d, count)
        return remote(
            src.at[pl.ds(pl.multiple_of(peer * size, 16), size)],
            (land_a, land_b, land_c)[level].at[i, d - 1],
            s_send.at[i, level, d - 1], s_recv.at[i, level, d - 1], device(peer),
        )

    def scatter_start(i, level):
        for d in range(1, groups[level][0]):
            scatter_copy(i, level, d).start()

    def scatter_end(i, level):
        count, index, _ = groups[level]
        lo, size = parts[level]
        for d in range(1, count):
            scatter_copy(i, level, d).wait_recv()
        src = (mine.at[i], sum_a.at[i], sum_b.at[i])[level]
        land = (land_a, land_b, land_c)[level]
        z = src[pl.ds(pl.multiple_of(index * size, 16), size)].astype(F32)
        for d in range(1, count):
            z = z + land[i, d - 1].astype(F32)
        if level < 2:
            (sum_a, sum_b)[level][i] = z.astype(BF16)
        else:
            (total1, total2)[i][pl.ds(pl.multiple_of(lo, 16), size)] = z.astype(BF16)

    def gather_copy(i, level, d):
        count, index, device = groups[level]
        lo, size = parts[level]
        part = (total1, total2)[i].at[pl.ds(pl.multiple_of(lo, 16), size)]
        return remote(
            part, part, t_send.at[i, level, d - 1], t_recv.at[i, level, d - 1], device(lax.rem(index + d, count))
        )

    def gather_start(i, level):
        for d in range(1, groups[level][0]):
            gather_copy(i, level, d).start()

    def gather_end(i, level):
        for d in range(1, groups[level][0]):
            gather_copy(i, level, d).wait_recv()

    def shifted(p):
        left, mid, right = (p[:, c * ch : (c + 1) * ch].reshape(rows, cw, ch) for c in range(3))
        pos = lax.broadcasted_iota(jnp.int32, (rows, cw, ch), 1)
        return (
            jnp.where(pos == 0, 0.0, pltpu.roll(left, 1, 1)) + mid
            + jnp.where(pos == cw - 1, 0.0, pltpu.roll(right, cw - 1, 1))
        )

    def conv_pair(k, w, t, epilogue):
        def x(j, b):
            return pads[k, t + j, pl.ds(b, rows)].reshape(rows * cw, ch)

        def taps(a, b):
            return jnp.concatenate([w[a, b, c] for c in range(3)], axis=1)

        def both(j, b):
            return jnp.concatenate([taps(j, b), taps(j - 1, b)], axis=1)

        def dot(xs, ws):
            return jnp.dot(
                jnp.concatenate(xs, axis=1), jnp.concatenate(ws, axis=0), preferred_element_type=F32
            )

        mid = [(j, b) for j in (1, 2) for b in range(3)]
        p = dot([x(j, b) for j, b in mid], [both(j, b) for j, b in mid])
        q0 = dot([x(0, b) for b in range(3)], [taps(0, b) for b in range(3)])
        q1 = dot([x(3, b) for b in range(3)], [taps(2, b) for b in range(3)])
        epilogue(t, shifted(p[:, : 3 * ch] + q0))
        epilogue(t + 1, shifted(p[:, 3 * ch :] + q1))

    inner = pl.ds(1, rows)

    def end0(t, z):
        sigma = jax.nn.sigmoid(z)
        slope1[t] = sigma * (1.0 + z * (1.0 - sigma))
        pads[1, HALO + t, inner] = (z * sigma).astype(BF16)

    def end1(t, z):
        sigma = jax.nn.sigmoid(z)
        crit_s[t] = (z * sigma).astype(BF16)
        delta = cotp[t].astype(F32) * (sigma * (1.0 + z * (1.0 - sigma)))
        pads[2, t, inner] = delta.astype(BF16)

    def end2(t, z):
        pads[3, t, inner] = (z * slope1[t]).astype(BF16)

    def end3(t, z):
        cg_s[t] = z.astype(BF16)

    def turn_weights():
        def one(i, c):
            a, b = i // 3, lax.rem(i, 3)
            for src, dst in ((w1v, w1t), (w2v, w2t)):
                for q in range(3):
                    dst[a, b, q] = src[2 - a, 2 - b, 2 - q].T
            return c
        lax.fori_loop(0, 9, one, 0)

    def turn_input(k, lo, n):
        def one(f, c):
            for r in range(rows + 2):
                xt[k, f, :, r * half : (r + 1) * half] = pads[k, f, r, pl.ds(own, half)].T
            return c
        lax.fori_loop(lo, lo + n, one, 0)

    def spread_delta(k, lo, n):
        def one(t, c):
            pos = lax.broadcasted_iota(jnp.int32, (cw, ch), 0)
            for r in range(rows):
                x = pads[k, t, r + 1].astype(F32)
                d3[t, r, :, 0:ch] = jnp.where(pos == cw - 1, 0.0, pltpu.roll(x, cw - 1, 0)).astype(BF16)
                d3[t, r, :, ch : 2 * ch] = pads[k, t, r + 1]
                d3[t, r, :, 2 * ch :] = jnp.where(pos == 0, 0.0, pltpu.roll(x, 1, 0)).astype(BF16)
            return c
        lax.fori_loop(lo, lo + n, one, 0)

    def weight_grad(k, ts, last, i):
        def one(a, c):
            z = None
            for t in ts:
                x = xt[k, t + a]
                left = jnp.concatenate([x[:, b * half : (b + rows) * half] for b in range(3)], axis=0)
                right = d3[t, :, pl.ds(own, half)].reshape(rows * half, 3 * ch)
                p = jnp.dot(left, right, preferred_element_type=F32)
                z = p if z is None else z + p
            if not last:
                acc[a] = z
            else:
                z = (z + acc[a]) * grad_scale
                for b in range(3):
                    for q in range(3):
                        at = pl.multiple_of(a * (9 * ch) + (b * 3 + q) * ch, ch)
                        mine[i, pl.ds(at, ch)] = z[b * ch : (b + 1) * ch, q * ch : (q + 1) * ch].astype(BF16)
            return c
        lax.fori_loop(0, 3, one, 0)

    for t in range(step):
        loads[2 * t].wait()
    for t in (1, 0):
        cross_copy(0, t).start()
    for t in range(step):
        loads[2 * t + 1].wait()

    def publish_clip(who, fs):
        @pl.when(who)
        def _():
            for f in fs:
                if f >= frames:
                    send_frame(0, f - frames)
                send_rows(0, f)

    publish_clip(second, (frames + 1, frames))
    publish_clip(first, (HALO + 1, HALO))
    for t in (1, 0):
        cross_copy(1, t).start()
    loads[2 * step].wait()
    loads[2 * step + 1].wait()
    turn_weights()
    for t in (1, 0):
        cross_copy(0, t).wait_recv()
        publish_clip(first, (HALO + step + t,))
        publish_clip(second, (HALO + t,))

    local_f = tuple(range(HALO, HALO + frames))
    local_b = tuple(range(frames))

    wait_rows(0, local_f)
    conv_pair(0, w1v, 2, end0)
    for t in (1, 0):
        send_frame(1, t)
        send_rows(1, frames + t)
    take_halo(0)
    conv_pair(0, w1v, 0, end0)
    for f in (HALO + 1, HALO):
        send_rows(1, f)
    turn_input(0, 0, frames + HALO)

    for t in range(step):
        loads[2 * step + 2 + t].wait()
        cross_copy(1, t).wait_recv()
    wait_rows(1, local_f)
    conv_pair(1, w2v, 2, end1)
    for t in (2, 3):
        send_rows(2, t)

    def send_out(i, who):
        @pl.when(who)
        def _():
            for t in range(step):
                out_copy(i, t).start()

    send_out(0, first)
    turn_input(1, HALO, frames)
    spread_delta(2, 2, 2)
    weight_grad(1, (2, 3), False, 1)
    take_halo(1)
    conv_pair(1, w2v, 0, end1)
    for t in (0, 1):
        send_frame(2, t)
        send_rows(2, t)
    send_out(0, second)
    for t in range(step):
        keep_copy(0, t).start()
    turn_input(1, 0, HALO)
    spread_delta(2, 0, 2)
    weight_grad(1, (0, 1), True, 1)
    scatter_start(1, 0)

    wait_rows(2, local_b)
    conv_pair(2, w2t, 0, end2)
    for t in (0, 1):
        send_frame(3, t)
        send_rows(3, t)
    scatter_end(1, 0)
    scatter_start(1, 1)
    spread_delta(3, 0, 2)
    weight_grad(0, (0, 1), False, 0)
    take_halo(2)
    conv_pair(2, w2t, 2, end2)
    for t in (2, 3):
        send_rows(3, t)
    spread_delta(3, 2, 2)
    weight_grad(0, (2, 3), True, 0)
    scatter_start(0, 0)
    scatter_end(1, 1)
    scatter_start(1, 2)

    wait_rows(3, local_b)
    scatter_end(0, 0)
    scatter_start(0, 1)
    conv_pair(3, w1t, 0, end3)
    send_out(1, second)
    scatter_end(1, 2)
    gather_start(1, 2)
    take_halo(3)
    conv_pair(3, w1t, 2, end3)
    send_out(1, first)
    for t in range(step):
        keep_copy(1, t).start()
    scatter_end(0, 1)
    scatter_start(0, 2)
    gather_end(1, 2)
    gather_start(1, 1)
    scatter_end(0, 2)
    gather_start(0, 2)
    gather_end(1, 1)
    gather_start(1, 0)
    gather_end(0, 2)
    gather_start(0, 1)
    gather_end(1, 0)
    gather_end(0, 1)
    gather_start(0, 0)
    gather_end(0, 0)

    for i in range(2):
        for t in range(step):
            cross_copy(i, t).wait_send()
            out_copy(i, t).wait()
            keep_copy(i, t).wait()
        for level in range(3):
            for d in range(1, groups[level][0]):
                scatter_copy(i, level, d).wait_send()
                gather_copy(i, level, d).wait_send()
    for k in range(4):
        fwd = k < 2

        @pl.when(later if fwd else earlier)
        def _():
            for t in range(HALO):
                frame_copy(k, t).wait_send()
        for f in range(frames + HALO):
            is_halo = f < HALO if fwd else f >= frames
            has = earlier if fwd else later
            for way, there in ((0, below), (1, above)):
                @pl.when(jnp.logical_and(there, has) if is_halo else there)
                def _():
                    row_copy(k, f, way).wait_send()


def on_device(n_frame, n_row, clip, first_kernel, second_kernel, cotangent):
    step, rows, width, ch = clip.shape
    grad_scale = 1.0 / float(step * n_frame * rows * n_row * width) ** 0.5
    n = n_frame * n_row
    frames, cw = 2 * step, width // 2 + MARGIN
    vmem, hbm = pl.BlockSpec(memory_space=pltpu.VMEM), pl.BlockSpec(memory_space=pl.ANY)
    weights = first_kernel.shape
    length = 27 * ch
    padded = -(-length // (16 * n)) * 16 * n
    counts = (2, n_row // 2 * 2, n_frame // 2)
    size_a = padded // counts[0]
    size_b = size_a // counts[1]
    size_c = size_b // counts[2]
    most = max(counts) - 1
    sems = pltpu.SemaphoreType.DMA
    block = (frames, rows, cw, ch)
    critic, clip_grad, t1, t2 = pl.pallas_call(
        functools.partial(kernel, n_frame, n_row, grad_scale),
        out_shape=(
            jax.ShapeDtypeStruct(clip.shape, BF16),
            jax.ShapeDtypeStruct(clip.shape, BF16),
            jax.ShapeDtypeStruct((padded, ch), BF16),
            jax.ShapeDtypeStruct((padded, ch), BF16),
        ),
        in_specs=[hbm] * 4,
        out_specs=(hbm, hbm, vmem, vmem),
        scratch_shapes=[
            pltpu.VMEM((4, frames + HALO, rows + 2, cw, ch), BF16),
            pltpu.VMEM((step, rows, cw, ch), BF16),
            pltpu.VMEM(block, BF16),
            pltpu.VMEM(block, BF16),
            pltpu.VMEM(block, BF16),
            pltpu.VMEM(block, F32),
            pltpu.VMEM(weights, BF16),
            pltpu.VMEM(weights, BF16),
            pltpu.VMEM(weights, BF16),
            pltpu.VMEM(weights, BF16),
            pltpu.VMEM((2, frames + HALO, ch, (rows + 2) * (width // 2)), BF16),
            pltpu.VMEM((frames, rows, cw, 3 * ch), BF16),
            pltpu.VMEM((3, 3 * ch, 3 * ch), F32),
            pltpu.VMEM((2, padded, ch), BF16),
            pltpu.VMEM((2, counts[0] - 1, size_a, ch), BF16),
            pltpu.VMEM((2, size_a, ch), BF16),
            pltpu.VMEM((2, counts[1] - 1, size_b, ch), BF16),
            pltpu.VMEM((2, size_b, ch), BF16),
            pltpu.VMEM((2, counts[2] - 1, size_c, ch), BF16),
            sems((3 * step + 2,)),
            sems((2, step)), sems((2, step)),
            sems((2, step)), sems((2, step)),
            sems((4, HALO)), sems((4, HALO)),
            sems((4, frames + HALO, 2)), sems((4, frames + HALO, 2)),
            sems((2, 3, most)), sems((2, 3, most)),
            sems((2, 3, most)), sems((2, 3, most)),
        ],
        compiler_params=pltpu.CompilerParams(
            collective_id=0, has_side_effects=True, vmem_limit_bytes=60 * 2**20
        ),
    )(clip, first_kernel, second_kernel, cotangent)
    g1, g2 = (t[:length].astype(F32).reshape(weights) for t in (t1, t2))
    return critic, clip_grad, g1, g2


def solution(mesh):
    placed = (P("frame", "row", None, None), P(), P(), P("frame", "row", None, None))
    return jax.shard_map(
        functools.partial(on_device, mesh.shape["frame"], mesh.shape["row"]),
        mesh=mesh,
        in_specs=placed,
        out_specs=(P("frame", "row", None, None), P("frame", "row", None, None), P(), P()),
        check_vma=False,
    )
```

```python
import functools

import jax
import jax.numpy as jnp
from jax import lax
from jax.experimental import pallas as pl
from jax.experimental.pallas import tpu as pltpu
from jax.sharding import PartitionSpec as P

MESH = pl.DeviceIdType.MESH
BF16, F32 = jnp.bfloat16, jnp.float32
MARGIN = 8
HALO = 2


def sum_groups(n_frame, n_row, me_f, me_r):
    pair, member = me_f // 2, lax.rem(me_f, 2)
    side, core = me_r // 2, lax.rem(me_r, 2)
    return (
        (2, core, lambda j: {"row": side * 2 + j}),
        (n_row // 2 * 2, side * 2 + member, lambda j: {"row": j // 2 * 2 + core, "frame": pair * 2 + lax.rem(j, 2)}),
        (n_frame // 2, pair, lambda j: {"frame": j * 2 + member}),
    )


def kernel(
    n_frame, n_row, grad_scale,
    clip, w1, w2, cot,
    critic, clip_grad, total1, total2,
    pads, cross, cotp, crit_s, cg_s, slope1, w1v, w2v, w1t, w2t, xt, d3, acc,
    mine, land_a, sum_a, land_b, sum_b, land_c,
    l_sem, x_send, x_recv, o_send, o_recv, f_send, f_recv, c_send, c_recv, r_send, r_recv,
    a_send, a_recv, b_send, b_recv, z_send, z_recv, ga_send, ga_recv, gb_send, gb_recv, gz_send, gz_recv,
):
    step, rows, width, ch = clip.shape
    half = width // 2
    cw = half + MARGIN
    frames = 2 * step
    me_f, me_r = lax.axis_index("frame"), lax.axis_index("row")
    member = lax.rem(me_f, 2)
    first, second = member == 0, member == 1
    later, earlier = me_f < n_frame - 2, me_f > 1
    below, above = me_r < n_row - 1, me_r > 0
    partner = {"frame": me_f + 1 - 2 * member}
    groups = sum_groups(n_frame, n_row, me_f, me_r)
    own = pl.multiple_of(member * MARGIN, MARGIN)
    odd = lax.rem(me_r, 2)
    facing = jnp.logical_or(jnp.logical_and(odd == 1, below), jnp.logical_and(odd == 0, above))
    mate, across = me_r + 1 - 2 * odd, me_r - 1 + 2 * odd

    def start_of(who):
        return pl.multiple_of(who * (half - MARGIN), MARGIN)

    barrier = pltpu.get_barrier_semaphore()
    for there, who in ((below, {"row": me_r + 1}), (above, {"row": me_r - 1})):
        @pl.when(there)
        def _():
            pl.semaphore_signal(barrier, inc=1, device_id=who, device_id_type=MESH)
    greeted = below.astype(jnp.int32) + above.astype(jnp.int32)
    for there, way in ((later, 2), (earlier, -2)):
        met = jnp.logical_and(there, facing)

        @pl.when(met)
        def _():
            who = {"frame": me_f + way, "row": across}
            pl.semaphore_signal(barrier, inc=1, device_id=who, device_id_type=MESH)
        greeted = greeted + met.astype(jnp.int32)
    for count, index, device in groups[1:]:
        for d in range(1, count):
            pl.semaphore_signal(barrier, inc=1, device_id=device(lax.rem(index + d, count)), device_id_type=MESH)
        greeted = greeted + (count - 1)

    loads = []
    for t in range(step):
        mine_at, other_at = pl.ds(start_of(member), cw), pl.ds(start_of(1 - member), cw)
        loads.append((clip.at[t, :, other_at], cross.at[t]))
        loads.append((clip.at[t, :, mine_at], pads.at[0, HALO + step * member + t, pl.ds(1, rows)]))
    loads.append((w1, w1v))
    loads.append((w2, w2v))
    for t in range(step):
        loads.append((cot.at[t, :, mine_at], cotp.at[step * member + t]))
    loads = [pltpu.make_async_copy(a, b, l_sem.at[i]) for i, (a, b) in enumerate(loads)]
    for load in loads:
        load.start()

    def zero(ref):
        ref[...] = jnp.zeros(ref.shape, ref.dtype)

    for k in range(4):
        @pl.when(jnp.logical_not(earlier if k < 2 else later))
        def _():
            for f in ((0, 1) if k < 2 else (frames, frames + 1)):
                zero(pads.at[k, f])

        @pl.when(jnp.logical_not(above))
        def _():
            for f in range(frames + HALO):
                zero(pads.at[k, f, 0])

        @pl.when(jnp.logical_not(below))
        def _():
            for f in range(frames + HALO):
                zero(pads.at[k, f, rows + 1])
    used = 27 * ch
    for i in range(2):
        mine[i, pl.ds(used, mine.shape[1] - used)] = jnp.zeros((mine.shape[1] - used, ch), BF16)

    pl.semaphore_wait(barrier, greeted)

    def remote(src, dst, send, recv, who):
        return pltpu.make_async_remote_copy(
            src_ref=src, dst_ref=dst, send_sem=send, recv_sem=recv, device_id=who, device_id_type=MESH
        )

    def cross_copy(i, t):
        if i == 0:
            src, dst = cross.at[t], pads.at[0, HALO + step * member + t, pl.ds(1, rows)]
        else:
            src, dst = cot.at[t, :, pl.ds(start_of(1 - member), cw)], cotp.at[step * member + t]
        return remote(src, dst, x_send.at[i, t], x_recv.at[i, t], partner)

    def out_copy(i, t):
        src, dst = ((crit_s, critic), (cg_s, clip_grad))[i]
        return remote(
            src.at[step * (1 - member) + t, :, pl.ds(own, half)],
            dst.at[t, :, pl.ds(pl.multiple_of(member * half, half), half)],
            o_send.at[i, t], o_recv.at[i, t], partner,
        )

    def keep_copy(i, t):
        src, dst = ((crit_s, critic), (cg_s, clip_grad))[i]
        return pltpu.make_async_copy(
            src.at[step * member + t, :, pl.ds(own, half)],
            dst.at[t, :, pl.ds(pl.multiple_of(member * half, half), half)],
            l_sem.at[i * step + t],
        )

    def frame_copy(k, t):
        fwd = k < 2
        src, dst = (frames + t, t) if fwd else (t, frames + t)
        return remote(
            pads.at[k, src, pl.ds(1, rows)], pads.at[k, dst, pl.ds(1, rows)],
            f_send.at[k, t], f_recv.at[k, t], {"frame": me_f + 2 if fwd else me_f - 2},
        )

    def row_copy(k, f, way):
        src, dst = ((rows, 0), (1, rows + 1))[way]
        return remote(
            pads.at[k, f, src], pads.at[k, f, dst],
            r_send.at[k, f, way], r_recv.at[k, f, way], {"row": me_r + 1 if way == 0 else me_r - 1},
        )

    def send_rows(k, f):
        @pl.when(below)
        def _():
            row_copy(k, f, 0).start()

        @pl.when(above)
        def _():
            row_copy(k, f, 1).start()

    def wait_rows(k, fs):
        for f in fs:
            @pl.when(above)
            def _():
                row_copy(k, f, 0).wait_recv()

            @pl.when(below)
            def _():
                row_copy(k, f, 1).wait_recv()

    def corner_copy(k, t):
        fwd = k < 2
        src, dst = (frames + t, t) if fwd else (t, frames + t)
        return remote(
            pads.at[k, src, 1 + odd * (rows - 1)], pads.at[k, dst, (1 - odd) * (rows + 1)],
            c_send.at[k, t], c_recv.at[k, t], {"frame": me_f + 2 if fwd else me_f - 2, "row": across},
        )

    def mate_copy(k, t):
        f = t if k < 2 else frames + t
        return remote(
            pads.at[k, f, rows - odd * (rows - 1)], pads.at[k, f, odd * (rows + 1)],
            r_send.at[k, f, 0], r_recv.at[k, f, 0], {"row": mate},
        )

    def send_frame(k, t):
        there = later if k < 2 else earlier

        @pl.when(there)
        def _():
            frame_copy(k, t).start()

        @pl.when(jnp.logical_and(there, facing))
        def _():
            corner_copy(k, t).start()

    def pass_halo(k, t):
        @pl.when(earlier if k < 2 else later)
        def _():
            frame_copy(k, t).wait_recv()
            mate_copy(k, t).start()

    def wait_halo(k):
        there = earlier if k < 2 else later

        @pl.when(there)
        def _():
            for t in range(HALO):
                mate_copy(k, t).wait_recv()

        @pl.when(jnp.logical_and(there, facing))
        def _():
            for t in range(HALO):
                corner_copy(k, t).wait_recv()

    (_, core, to_core), (n_b, in_b, to_b), (n_c, in_c, to_c) = groups
    half_rows = sum_a.shape[1]
    piece = half_rows // (n_b * n_c)

    def aligned(x):
        return pl.multiple_of(x, 16)

    def block(q):
        return aligned(q * (n_b * piece))

    def a_copy(i):
        src = mine.at[i, pl.ds(aligned((1 - core) * half_rows), half_rows)]
        return remote(src, land_a.at[i], a_send.at[i], a_recv.at[i], to_core(1 - core))

    def b_copy(i, d, e):
        peer = lax.rem(in_b + e, n_b)
        src = sum_a.at[i, pl.ds(aligned(block(lax.rem(in_c + d, n_c)) + peer * piece), piece)]
        return remote(src, land_b.at[i, d, e - 1], b_send.at[i, d, e - 1], b_recv.at[i, d, e - 1], to_b(peer))

    def z_copy(i, d):
        peer = lax.rem(in_c + d, n_c)
        return remote(sum_b.at[i, d - 1], land_c.at[i, d - 1], z_send.at[i, d - 1], z_recv.at[i, d - 1], to_c(peer))

    order = tuple(range(n_c - 1, 0, -1))

    def sum_phase_a(i):
        a_copy(i).start()

    def sum_phase_b(i):
        a_copy(i).wait_recv()
        kept = mine[i, pl.ds(aligned(core * half_rows), half_rows)].astype(F32)
        sum_a[i] = (kept + land_a[i].astype(F32)).astype(BF16)
        for d in order + (0,):
            for e in range(1, n_b):
                b_copy(i, d, e).start()

    def plane_sum(i, d):
        for e in range(1, n_b):
            b_copy(i, d, e).wait_recv()
        z = sum_a[i, pl.ds(aligned(block(lax.rem(in_c + d, n_c)) + in_b * piece), piece)].astype(F32)
        for e in range(1, n_b):
            z = z + land_b[i, d, e - 1].astype(F32)
        return z

    def sum_phase_c(i, ds):
        for d in ds:
            sum_b[i, d - 1] = plane_sum(i, d).astype(BF16)
            z_copy(i, d).start()

    def total_at(i, q, j, n):
        lo = aligned(core * half_rows + block(q) + j * piece)
        return (total1, total2)[i].at[pl.ds(lo, n)]

    def gz_copy(i, d):
        part = total_at(i, in_c, in_b, piece)
        return remote(part, part, gz_send.at[i, d - 1], gz_recv.at[i, d - 1], to_c(lax.rem(in_c + d, n_c)))

    def source(d):
        return lax.rem(in_c + n_c - d, n_c)

    def gb_copy(i, d, e):
        part = total_at(i, source(d), in_b, piece)
        return remote(
            part, part, gb_send.at[i, d, e - 1], gb_recv.at[i, d, e - 1], to_b(lax.rem(in_b + e, n_b))
        )

    def ga_copy(i, d):
        part = total_at(i, source(d), 0, n_b * piece)
        return remote(part, part, ga_send.at[i, d], ga_recv.at[i, d], to_core(1 - core))

    def total_phase_z(i):
        z = plane_sum(i, 0)
        for d in range(1, n_c):
            z_copy(i, d).wait_recv()
            z = z + land_c[i, d - 1].astype(F32)
        total_at(i, in_c, in_b, piece)[...] = z.astype(BF16)
        for d in order:
            gz_copy(i, d).start()
        for e in range(1, n_b):
            gb_copy(i, 0, e).start()

    def total_phase_b(i):
        for d in range(1, n_c):
            gz_copy(i, d).wait_recv()
            for e in range(1, n_b):
                gb_copy(i, d, e).start()

    def total_phase_a(i):
        for d in range(n_c):
            for e in range(1, n_b):
                gb_copy(i, d, e).wait_recv()
            ga_copy(i, d).start()

    def total_phase_end(i):
        for d in range(n_c):
            ga_copy(i, d).wait_recv()

    def shifted(p):
        left, mid, right = (p[:, c * ch : (c + 1) * ch].reshape(rows, cw, ch) for c in range(3))
        pos = lax.broadcasted_iota(jnp.int32, (rows, cw, ch), 1)
        return (
            jnp.where(pos == 0, 0.0, pltpu.roll(left, 1, 1)) + mid
            + jnp.where(pos == cw - 1, 0.0, pltpu.roll(right, cw - 1, 1))
        )

    def conv_pair(k, w, t, epilogue):
        def x(j, b):
            return pads[k, t + j, pl.ds(b, rows)].reshape(rows * cw, ch)

        def taps(a, b):
            return jnp.concatenate([w[a, b, c] for c in range(3)], axis=1)

        def both(j, b):
            return jnp.concatenate([taps(j, b), taps(j - 1, b)], axis=1)

        def dot(xs, ws):
            return jnp.dot(
                jnp.concatenate(xs, axis=1), jnp.concatenate(ws, axis=0), preferred_element_type=F32
            )

        mid = [(j, b) for j in (1, 2) for b in range(3)]
        p = dot([x(j, b) for j, b in mid], [both(j, b) for j, b in mid])
        q0 = dot([x(0, b) for b in range(3)], [taps(0, b) for b in range(3)])
        q1 = dot([x(3, b) for b in range(3)], [taps(2, b) for b in range(3)])
        epilogue(t, shifted(p[:, : 3 * ch] + q0))
        epilogue(t + 1, shifted(p[:, 3 * ch :] + q1))

    inner = pl.ds(1, rows)

    def end0(t, z):
        sigma = jax.nn.sigmoid(z)
        slope1[t] = sigma * (1.0 + z * (1.0 - sigma))
        pads[1, HALO + t, inner] = (z * sigma).astype(BF16)

    def end1(t, z):
        sigma = jax.nn.sigmoid(z)
        crit_s[t] = (z * sigma).astype(BF16)
        delta = cotp[t].astype(F32) * (sigma * (1.0 + z * (1.0 - sigma)))
        pads[2, t, inner] = delta.astype(BF16)

    def end2(t, z):
        pads[3, t, inner] = (z * slope1[t]).astype(BF16)

    def end3(t, z):
        cg_s[t] = z.astype(BF16)

    def turn_weights():
        def one(i, c):
            a, b = i // 3, lax.rem(i, 3)
            for src, dst in ((w1v, w1t), (w2v, w2t)):
                for q in range(3):
                    dst[a, b, q] = src[2 - a, 2 - b, 2 - q].T
            return c
        lax.fori_loop(0, 9, one, 0)

    def turn_input(k, lo, n):
        def one(f, c):
            for r in range(rows + 2):
                xt[k, f, :, r * half : (r + 1) * half] = pads[k, f, r, pl.ds(own, half)].T
            return c
        lax.fori_loop(lo, lo + n, one, 0)

    def spread_delta(k, lo, n):
        def one(t, c):
            pos = lax.broadcasted_iota(jnp.int32, (cw, ch), 0)
            for r in range(rows):
                x = pads[k, t, r + 1].astype(F32)
                d3[t, r, :, 0:ch] = jnp.where(pos == cw - 1, 0.0, pltpu.roll(x, cw - 1, 0)).astype(BF16)
                d3[t, r, :, ch : 2 * ch] = pads[k, t, r + 1]
                d3[t, r, :, 2 * ch :] = jnp.where(pos == 0, 0.0, pltpu.roll(x, 1, 0)).astype(BF16)
            return c
        lax.fori_loop(lo, lo + n, one, 0)

    def weight_grad(k, ts, last, i):
        def one(a, c):
            z = None
            for t in ts:
                x = xt[k, t + a]
                left = jnp.concatenate([x[:, b * half : (b + rows) * half] for b in range(3)], axis=0)
                right = d3[t, :, pl.ds(own, half)].reshape(rows * half, 3 * ch)
                p = jnp.dot(left, right, preferred_element_type=F32)
                z = p if z is None else z + p
            if not last:
                acc[a] = z
            else:
                z = (z + acc[a]) * grad_scale
                for b in range(3):
                    for q in range(3):
                        at = pl.multiple_of(a * (9 * ch) + (b * 3 + q) * ch, ch)
                        mine[i, pl.ds(at, ch)] = z[b * ch : (b + 1) * ch, q * ch : (q + 1) * ch].astype(BF16)
            return c
        lax.fori_loop(0, 3, one, 0)

    for t in range(step):
        loads[2 * t].wait()
    for t in (1, 0):
        cross_copy(0, t).start()
    for t in range(step):
        loads[2 * t + 1].wait()

    def publish_clip(who, fs):
        @pl.when(who)
        def _():
            for f in fs:
                if f >= frames:
                    send_frame(0, f - frames)
                send_rows(0, f)

    publish_clip(second, (frames + 1, frames))
    publish_clip(first, (HALO + 1, HALO))
    for t in (1, 0):
        cross_copy(1, t).start()
    loads[2 * step].wait()
    loads[2 * step + 1].wait()
    turn_weights()
    for t in (1, 0):
        cross_copy(0, t).wait_recv()
        publish_clip(first, (HALO + step + t,))
        publish_clip(second, (HALO + t,))

    local_f = tuple(range(HALO, HALO + frames))
    local_b = tuple(range(frames))

    wait_rows(0, local_f)
    conv_pair(0, w1v, 2, end0)
    for t in (1, 0):
        send_frame(1, t)
        send_rows(1, frames + t)
    pass_halo(0, 1)
    pass_halo(0, 0)
    wait_halo(0)
    conv_pair(0, w1v, 0, end0)
    for f in (HALO + 1, HALO):
        send_rows(1, f)
    turn_input(0, 0, frames + HALO)

    for t in range(step):
        loads[2 * step + 2 + t].wait()
        cross_copy(1, t).wait_recv()
    wait_rows(1, local_f)
    pass_halo(1, 1)
    conv_pair(1, w2v, 2, end1)
    for t in (2, 3):
        send_rows(2, t)

    def send_out(i, who):
        @pl.when(who)
        def _():
            for t in range(step):
                out_copy(i, t).start()

    send_out(0, first)
    pass_halo(1, 0)
    turn_input(1, HALO, frames)
    spread_delta(2, 2, 2)
    weight_grad(1, (2, 3), False, 1)
    wait_halo(1)
    conv_pair(1, w2v, 0, end1)
    for t in (0, 1):
        send_frame(2, t)
        send_rows(2, t)
    send_out(0, second)
    for t in range(step):
        keep_copy(0, t).start()
    turn_input(1, 0, HALO)
    spread_delta(2, 0, 2)
    weight_grad(1, (0, 1), True, 1)
    sum_phase_a(1)

    wait_rows(2, local_b)
    conv_pair(2, w2t, 0, end2)
    for t in (0, 1):
        send_frame(3, t)
        send_rows(3, t)
    sum_phase_b(1)
    pass_halo(2, 0)
    spread_delta(3, 0, 2)
    weight_grad(0, (0, 1), False, 0)
    pass_halo(2, 1)
    sum_phase_c(1, order[:1])
    wait_halo(2)
    conv_pair(2, w2t, 2, end2)
    for t in (2, 3):
        send_rows(3, t)
    sum_phase_c(1, order[1:])
    spread_delta(3, 2, 2)
    weight_grad(0, (2, 3), True, 0)
    sum_phase_a(0)
    total_phase_z(1)

    pass_halo(3, 0)
    pass_halo(3, 1)
    sum_phase_b(0)
    total_phase_b(1)
    wait_rows(3, local_b)
    conv_pair(3, w1t, 0, end3)
    send_out(1, second)
    wait_halo(3)
    conv_pair(3, w1t, 2, end3)
    send_out(1, first)
    for t in range(step):
        keep_copy(1, t).start()
    sum_phase_c(0, order)
    total_phase_z(0)
    total_phase_a(1)
    total_phase_b(0)
    total_phase_a(0)
    total_phase_end(1)
    total_phase_end(0)

    for i in range(2):
        for t in range(step):
            cross_copy(i, t).wait_send()
            out_copy(i, t).wait()
            keep_copy(i, t).wait()
        a_copy(i).wait_send()
        for d in range(n_c):
            ga_copy(i, d).wait_send()
            for e in range(1, n_b):
                b_copy(i, d, e).wait_send()
                gb_copy(i, d, e).wait_send()
        for d in range(1, n_c):
            z_copy(i, d).wait_send()
            gz_copy(i, d).wait_send()
    for k in range(4):
        fwd = k < 2

        @pl.when(later if fwd else earlier)
        def _():
            for t in range(HALO):
                frame_copy(k, t).wait_send()

        @pl.when(jnp.logical_and(later if fwd else earlier, facing))
        def _():
            for t in range(HALO):
                corner_copy(k, t).wait_send()

        @pl.when(earlier if fwd else later)
        def _():
            for t in range(HALO):
                mate_copy(k, t).wait_send()
        for f in local_f if fwd else local_b:
            for way, there in ((0, below), (1, above)):
                @pl.when(there)
                def _():
                    row_copy(k, f, way).wait_send()


def on_device(n_frame, n_row, clip, first_kernel, second_kernel, cotangent):
    step, rows, width, ch = clip.shape
    grad_scale = 1.0 / float(step * n_frame * rows * n_row * width) ** 0.5
    n = n_frame * n_row
    frames, cw = 2 * step, width // 2 + MARGIN
    vmem, hbm = pl.BlockSpec(memory_space=pltpu.VMEM), pl.BlockSpec(memory_space=pl.ANY)
    weights = first_kernel.shape
    length = 27 * ch
    padded = -(-length // (16 * n)) * 16 * n
    counts = (2, n_row // 2 * 2, n_frame // 2)
    size_a = padded // counts[0]
    piece = size_a // (counts[1] * counts[2])
    sems = pltpu.SemaphoreType.DMA
    block = (frames, rows, cw, ch)
    critic, clip_grad, t1, t2 = pl.pallas_call(
        functools.partial(kernel, n_frame, n_row, grad_scale),
        out_shape=(
            jax.ShapeDtypeStruct(clip.shape, BF16),
            jax.ShapeDtypeStruct(clip.shape, BF16),
            jax.ShapeDtypeStruct((padded, ch), BF16),
            jax.ShapeDtypeStruct((padded, ch), BF16),
        ),
        in_specs=[hbm] * 4,
        out_specs=(hbm, hbm, vmem, vmem),
        scratch_shapes=[
            pltpu.VMEM((4, frames + HALO, rows + 2, cw, ch), BF16),
            pltpu.VMEM((step, rows, cw, ch), BF16),
            pltpu.VMEM(block, BF16),
            pltpu.VMEM(block, BF16),
            pltpu.VMEM(block, BF16),
            pltpu.VMEM(block, F32),
            pltpu.VMEM(weights, BF16),
            pltpu.VMEM(weights, BF16),
            pltpu.VMEM(weights, BF16),
            pltpu.VMEM(weights, BF16),
            pltpu.VMEM((2, frames + HALO, ch, (rows + 2) * (width // 2)), BF16),
            pltpu.VMEM((frames, rows, cw, 3 * ch), BF16),
            pltpu.VMEM((3, 3 * ch, 3 * ch), F32),
            pltpu.VMEM((2, padded, ch), BF16),
            pltpu.VMEM((2, size_a, ch), BF16),
            pltpu.VMEM((2, size_a, ch), BF16),
            pltpu.VMEM((2, counts[2], counts[1] - 1, piece, ch), BF16),
            pltpu.VMEM((2, counts[2] - 1, piece, ch), BF16),
            pltpu.VMEM((2, counts[2] - 1, piece, ch), BF16),
            sems((3 * step + 2,)),
            sems((2, step)), sems((2, step)),
            sems((2, step)), sems((2, step)),
            sems((4, HALO)), sems((4, HALO)),
            sems((4, HALO)), sems((4, HALO)),
            sems((4, frames + HALO, 2)), sems((4, frames + HALO, 2)),
            sems((2,)), sems((2,)),
            sems((2, counts[2], counts[1] - 1)), sems((2, counts[2], counts[1] - 1)),
            sems((2, counts[2] - 1)), sems((2, counts[2] - 1)),
            sems((2, counts[2])), sems((2, counts[2])),
            sems((2, counts[2], counts[1] - 1)), sems((2, counts[2], counts[1] - 1)),
            sems((2, counts[2] - 1)), sems((2, counts[2] - 1)),
        ],
        compiler_params=pltpu.CompilerParams(
            collective_id=0, has_side_effects=True, vmem_limit_bytes=60 * 2**20
        ),
    )(clip, first_kernel, second_kernel, cotangent)
    g1, g2 = (t[:length].astype(F32).reshape(weights) for t in (t1, t2))
    return critic, clip_grad, g1, g2


def solution(mesh):
    placed = (P("frame", "row", None, None), P(), P(), P("frame", "row", None, None))
    return jax.shard_map(
        functools.partial(on_device, mesh.shape["frame"], mesh.shape["row"]),
        mesh=mesh,
        in_specs=placed,
        out_specs=(P("frame", "row", None, None), P("frame", "row", None, None), P(), P()),
        check_vma=False,
    )
```

```python
import functools

import jax
import jax.numpy as jnp
from jax import lax
from jax.experimental import pallas as pl
from jax.experimental.pallas import tpu as pltpu
from jax.sharding import PartitionSpec as P

MESH = pl.DeviceIdType.MESH
BF16, F32 = jnp.bfloat16, jnp.float32
MARGIN = 8
HALO = 2


def sum_groups(n_frame, n_row, me_f, me_r):
    side, core = me_r // 2, lax.rem(me_r, 2)
    return (
        (2, core, lambda j: {"row": side * 2 + j}),
        (n_row // 2, side, lambda j: {"row": j * 2 + core}),
        (n_frame, me_f, lambda j: {"frame": j}),
    )


def kernel(
    n_frame, n_row, grad_scale,
    clip, w1, w2, cot,
    critic, clip_grad, total1, total2,
    pads, cross, cotp, crit_s, cg_s, slope1, w1v, w2v, w1t, w2t, xt, d3, acc,
    mine, land_a, sum_a, land_b, sum_b, land_c,
    l_sem, x_send, x_recv, o_send, o_recv, f_send, f_recv, c_send, c_recv, r_send, r_recv,
    a_send, a_recv, b_send, b_recv, z_send, z_recv, ga_send, ga_recv, gb_send, gb_recv, gz_send, gz_recv,
):
    step, rows, width, ch = clip.shape
    half = width // 2
    cw = half + MARGIN
    frames = 2 * step
    me_f, me_r = lax.axis_index("frame"), lax.axis_index("row")
    member = lax.rem(me_f, 2)
    first, second = member == 0, member == 1
    later, earlier = me_f < n_frame - 2, me_f > 1
    below, above = me_r < n_row - 1, me_r > 0
    partner = {"frame": me_f + 1 - 2 * member}
    groups = sum_groups(n_frame, n_row, me_f, me_r)
    own = pl.multiple_of(member * MARGIN, MARGIN)
    odd = lax.rem(me_r, 2)
    facing = jnp.logical_or(jnp.logical_and(odd == 1, below), jnp.logical_and(odd == 0, above))
    mate, across = me_r + 1 - 2 * odd, me_r - 1 + 2 * odd

    def start_of(who):
        return pl.multiple_of(who * (half - MARGIN), MARGIN)

    barrier = pltpu.get_barrier_semaphore()
    for there, who in ((below, {"row": me_r + 1}), (above, {"row": me_r - 1})):
        @pl.when(there)
        def _():
            pl.semaphore_signal(barrier, inc=1, device_id=who, device_id_type=MESH)
    greeted = below.astype(jnp.int32) + above.astype(jnp.int32)
    for there, way in ((later, 2), (earlier, -2)):
        met = jnp.logical_and(there, facing)

        @pl.when(met)
        def _():
            who = {"frame": me_f + way, "row": across}
            pl.semaphore_signal(barrier, inc=1, device_id=who, device_id_type=MESH)
        greeted = greeted + met.astype(jnp.int32)
    for count, index, device in groups[1:]:
        for d in range(1, count):
            pl.semaphore_signal(barrier, inc=1, device_id=device(lax.rem(index + d, count)), device_id_type=MESH)
        greeted = greeted + (count - 1)

    loads = []
    for t in range(step):
        mine_at, other_at = pl.ds(start_of(member), cw), pl.ds(start_of(1 - member), cw)
        loads.append((clip.at[t, :, other_at], cross.at[t]))
        loads.append((clip.at[t, :, mine_at], pads.at[0, HALO + step * member + t, pl.ds(1, rows)]))
    loads.append((w1, w1v))
    loads.append((w2, w2v))
    for t in range(step):
        loads.append((cot.at[t, :, mine_at], cotp.at[step * member + t]))
    loads = [pltpu.make_async_copy(a, b, l_sem.at[i]) for i, (a, b) in enumerate(loads)]
    for load in loads:
        load.start()

    def zero(ref):
        ref[...] = jnp.zeros(ref.shape, ref.dtype)

    for k in range(4):
        @pl.when(jnp.logical_not(earlier if k < 2 else later))
        def _():
            for f in ((0, 1) if k < 2 else (frames, frames + 1)):
                zero(pads.at[k, f])

        @pl.when(jnp.logical_not(above))
        def _():
            for f in range(frames + HALO):
                zero(pads.at[k, f, 0])

        @pl.when(jnp.logical_not(below))
        def _():
            for f in range(frames + HALO):
                zero(pads.at[k, f, rows + 1])
    used = 27 * ch
    for i in range(2):
        mine[i, pl.ds(used, mine.shape[1] - used)] = jnp.zeros((mine.shape[1] - used, ch), BF16)

    pl.semaphore_wait(barrier, greeted)

    def remote(src, dst, send, recv, who):
        return pltpu.make_async_remote_copy(
            src_ref=src, dst_ref=dst, send_sem=send, recv_sem=recv, device_id=who, device_id_type=MESH
        )

    def cross_copy(i, t):
        if i == 0:
            src, dst = cross.at[t], pads.at[0, HALO + step * member + t, pl.ds(1, rows)]
        else:
            src, dst = cot.at[t, :, pl.ds(start_of(1 - member), cw)], cotp.at[step * member + t]
        return remote(src, dst, x_send.at[i, t], x_recv.at[i, t], partner)

    def out_copy(i, t):
        src, dst = ((crit_s, critic), (cg_s, clip_grad))[i]
        return remote(
            src.at[step * (1 - member) + t, :, pl.ds(own, half)],
            dst.at[t, :, pl.ds(pl.multiple_of(member * half, half), half)],
            o_send.at[i, t], o_recv.at[i, t], partner,
        )

    def keep(i):
        src, dst = ((crit_s, critic), (cg_s, clip_grad))[i]
        for t in range(step):
            dst[t, :, pl.ds(pl.multiple_of(member * half, half), half)] = src[step * member + t, :, pl.ds(own, half)]

    def frame_copy(k, t):
        fwd = k < 2
        src, dst = (frames + t, t) if fwd else (t, frames + t)
        return remote(
            pads.at[k, src, pl.ds(1, rows)], pads.at[k, dst, pl.ds(1, rows)],
            f_send.at[k, t], f_recv.at[k, t], {"frame": me_f + 2 if fwd else me_f - 2},
        )

    def row_copy(k, f, way):
        src, dst = ((rows, 0), (1, rows + 1))[way]
        return remote(
            pads.at[k, f, src], pads.at[k, f, dst],
            r_send.at[k, f, way], r_recv.at[k, f, way], {"row": me_r + 1 if way == 0 else me_r - 1},
        )

    def send_rows(k, f):
        @pl.when(below)
        def _():
            row_copy(k, f, 0).start()

        @pl.when(above)
        def _():
            row_copy(k, f, 1).start()

    def wait_rows(k, fs):
        for f in fs:
            @pl.when(above)
            def _():
                row_copy(k, f, 0).wait_recv()

            @pl.when(below)
            def _():
                row_copy(k, f, 1).wait_recv()

    def corner_copy(k, t):
        fwd = k < 2
        src, dst = (frames + t, t) if fwd else (t, frames + t)
        return remote(
            pads.at[k, src, 1 + odd * (rows - 1)], pads.at[k, dst, (1 - odd) * (rows + 1)],
            c_send.at[k, t], c_recv.at[k, t], {"frame": me_f + 2 if fwd else me_f - 2, "row": across},
        )

    def mate_copy(k, t):
        f = t if k < 2 else frames + t
        return remote(
            pads.at[k, f, rows - odd * (rows - 1)], pads.at[k, f, odd * (rows + 1)],
            r_send.at[k, f, 0], r_recv.at[k, f, 0], {"row": mate},
        )

    def send_frame(k, t):
        there = later if k < 2 else earlier

        @pl.when(there)
        def _():
            frame_copy(k, t).start()

        @pl.when(jnp.logical_and(there, facing))
        def _():
            corner_copy(k, t).start()

    def pass_halo(k, t):
        @pl.when(earlier if k < 2 else later)
        def _():
            frame_copy(k, t).wait_recv()
            mate_copy(k, t).start()

    def wait_halo(k):
        there = earlier if k < 2 else later

        @pl.when(there)
        def _():
            for t in range(HALO):
                mate_copy(k, t).wait_recv()

        @pl.when(jnp.logical_and(there, facing))
        def _():
            for t in range(HALO):
                corner_copy(k, t).wait_recv()

    (_, core, to_core), (n_b, in_b, to_b), (n_c, in_c, to_c) = groups
    half_rows = sum_a.shape[1]
    piece = half_rows // (n_b * n_c)

    def aligned(x):
        return pl.multiple_of(x, 16)

    def block(q):
        return aligned(q * (n_b * piece))

    def a_copy(i):
        src = mine.at[i, pl.ds(aligned((1 - core) * half_rows), half_rows)]
        return remote(src, land_a.at[i], a_send.at[i], a_recv.at[i], to_core(1 - core))

    def b_copy(i, d, e):
        peer = lax.rem(in_b + e, n_b)
        src = sum_a.at[i, pl.ds(aligned(block(lax.rem(in_c + d, n_c)) + peer * piece), piece)]
        return remote(src, land_b.at[i, d, e - 1], b_send.at[i, d, e - 1], b_recv.at[i, d, e - 1], to_b(peer))

    def z_copy(i, d):
        peer = lax.rem(in_c + d, n_c)
        return remote(sum_b.at[i, d - 1], land_c.at[i, d - 1], z_send.at[i, d - 1], z_recv.at[i, d - 1], to_c(peer))

    near = sorted(range(1, n_c), key=lambda d: min(d, n_c - d))
    order = tuple(reversed(near))

    def sum_phase_a(i):
        a_copy(i).start()

    def sum_phase_b(i):
        a_copy(i).wait_recv()
        kept = mine[i, pl.ds(aligned(core * half_rows), half_rows)].astype(F32)
        sum_a[i] = (kept + land_a[i].astype(F32)).astype(BF16)
        for d in order + (0,):
            for e in range(1, n_b):
                b_copy(i, d, e).start()

    def plane_sum(i, d):
        for e in range(1, n_b):
            b_copy(i, d, e).wait_recv()
        z = sum_a[i, pl.ds(aligned(block(lax.rem(in_c + d, n_c)) + in_b * piece), piece)].astype(F32)
        for e in range(1, n_b):
            z = z + land_b[i, d, e - 1].astype(F32)
        return z

    def sum_phase_c(i, ds):
        for d in ds:
            sum_b[i, d - 1] = plane_sum(i, d).astype(BF16)
            z_copy(i, d).start()

    def total_at(i, q, j, n):
        lo = aligned(core * half_rows + block(q) + j * piece)
        return (total1, total2)[i].at[pl.ds(lo, n)]

    def gz_copy(i, d):
        part = total_at(i, in_c, in_b, piece)
        return remote(part, part, gz_send.at[i, d - 1], gz_recv.at[i, d - 1], to_c(lax.rem(in_c + d, n_c)))

    def source(d):
        return lax.rem(in_c + n_c - d, n_c)

    def gb_copy(i, d, e):
        part = total_at(i, source(d), in_b, piece)
        return remote(
            part, part, gb_send.at[i, d, e - 1], gb_recv.at[i, d, e - 1], to_b(lax.rem(in_b + e, n_b))
        )

    def ga_copy(i, d):
        part = total_at(i, source(d), 0, n_b * piece)
        return remote(part, part, ga_send.at[i, d], ga_recv.at[i, d], to_core(1 - core))

    def total_phase_z(i):
        z = plane_sum(i, 0)
        for d in range(1, n_c):
            z_copy(i, d).wait_recv()
            z = z + land_c[i, d - 1].astype(F32)
        total_at(i, in_c, in_b, piece)[...] = z.astype(BF16)
        for d in order:
            gz_copy(i, d).start()
        for e in range(1, n_b):
            gb_copy(i, 0, e).start()

    def total_phase_b(i):
        for d in near:
            gz_copy(i, d).wait_recv()
            for e in range(1, n_b):
                gb_copy(i, d, e).start()

    def total_phase_a(i):
        for d in [0] + near:
            for e in range(1, n_b):
                gb_copy(i, d, e).wait_recv()
            ga_copy(i, d).start()

    def total_phase_end(i):
        for d in range(n_c):
            ga_copy(i, d).wait_recv()

    def shifted(p):
        left, mid, right = (p[:, c * ch : (c + 1) * ch].reshape(rows, cw, ch) for c in range(3))
        pos = lax.broadcasted_iota(jnp.int32, (rows, cw, ch), 1)
        return (
            jnp.where(pos == 0, 0.0, pltpu.roll(left, 1, 1)) + mid
            + jnp.where(pos == cw - 1, 0.0, pltpu.roll(right, cw - 1, 1))
        )

    def conv_pair(k, w, t, epilogue):
        def x(j, b):
            return pads[k, t + j, pl.ds(b, rows)].reshape(rows * cw, ch)

        def taps(a, b):
            return jnp.concatenate([w[a, b, c] for c in range(3)], axis=1)

        def both(j, b):
            return jnp.concatenate([taps(j, b), taps(j - 1, b)], axis=1)

        def dot(xs, ws):
            return jnp.dot(
                jnp.concatenate(xs, axis=1), jnp.concatenate(ws, axis=0), preferred_element_type=F32
            )

        mid = [(j, b) for j in (1, 2) for b in range(3)]
        p = dot([x(j, b) for j, b in mid], [both(j, b) for j, b in mid])
        q0 = dot([x(0, b) for b in range(3)], [taps(0, b) for b in range(3)])
        q1 = dot([x(3, b) for b in range(3)], [taps(2, b) for b in range(3)])
        epilogue(t, shifted(p[:, : 3 * ch] + q0))
        epilogue(t + 1, shifted(p[:, 3 * ch :] + q1))

    inner = pl.ds(1, rows)

    def end0(t, z):
        sigma = jax.nn.sigmoid(z)
        slope1[t] = sigma * (1.0 + z * (1.0 - sigma))
        pads[1, HALO + t, inner] = (z * sigma).astype(BF16)

    def end1(t, z):
        sigma = jax.nn.sigmoid(z)
        crit_s[t] = (z * sigma).astype(BF16)
        delta = cotp[t].astype(F32) * (sigma * (1.0 + z * (1.0 - sigma)))
        pads[2, t, inner] = delta.astype(BF16)

    def end2(t, z):
        pads[3, t, inner] = (z * slope1[t]).astype(BF16)

    def end3(t, z):
        cg_s[t] = z.astype(BF16)

    def turn_weights():
        def one(i, c):
            a, b = i // 3, lax.rem(i, 3)
            for src, dst in ((w1v, w1t), (w2v, w2t)):
                for q in range(3):
                    dst[a, b, q] = src[2 - a, 2 - b, 2 - q].T
            return c
        lax.fori_loop(0, 9, one, 0)

    def turn_input(k, lo, n):
        def one(f, c):
            for r in range(rows + 2):
                xt[k, f, :, r * half : (r + 1) * half] = pads[k, f, r, pl.ds(own, half)].T
            return c
        lax.fori_loop(lo, lo + n, one, 0)

    def spread_delta(k, lo, n):
        def one(t, c):
            pos = lax.broadcasted_iota(jnp.int32, (cw, ch), 0)
            for r in range(rows):
                x = pads[k, t, r + 1].astype(F32)
                d3[t, r, :, 0:ch] = jnp.where(pos == cw - 1, 0.0, pltpu.roll(x, cw - 1, 0)).astype(BF16)
                d3[t, r, :, ch : 2 * ch] = pads[k, t, r + 1]
                d3[t, r, :, 2 * ch :] = jnp.where(pos == 0, 0.0, pltpu.roll(x, 1, 0)).astype(BF16)
            return c
        lax.fori_loop(lo, lo + n, one, 0)

    def weight_grad(k, ts, last, i):
        def one(a, c):
            z = None
            for t in ts:
                x = xt[k, t + a]
                left = jnp.concatenate([x[:, b * half : (b + rows) * half] for b in range(3)], axis=0)
                right = d3[t, :, pl.ds(own, half)].reshape(rows * half, 3 * ch)
                p = jnp.dot(left, right, preferred_element_type=F32)
                z = p if z is None else z + p
            if not last:
                acc[a] = z
            else:
                z = (z + acc[a]) * grad_scale
                for b in range(3):
                    for q in range(3):
                        at = pl.multiple_of(a * (9 * ch) + (b * 3 + q) * ch, ch)
                        mine[i, pl.ds(at, ch)] = z[b * ch : (b + 1) * ch, q * ch : (q + 1) * ch].astype(BF16)
            return c
        lax.fori_loop(0, 3, one, 0)

    for t in range(step):
        loads[2 * t].wait()
    for t in (1, 0):
        cross_copy(0, t).start()
    for t in range(step):
        loads[2 * t + 1].wait()

    def publish_clip(who, fs):
        @pl.when(who)
        def _():
            for f in fs:
                if f >= frames:
                    send_frame(0, f - frames)
                send_rows(0, f)

    publish_clip(second, (frames + 1, frames))
    publish_clip(first, (HALO + 1, HALO))
    for t in (1, 0):
        cross_copy(1, t).start()
    loads[2 * step].wait()
    loads[2 * step + 1].wait()
    turn_weights()
    for t in (1, 0):
        cross_copy(0, t).wait_recv()
        publish_clip(first, (HALO + step + t,))
        publish_clip(second, (HALO + t,))

    local_f = tuple(range(HALO, HALO + frames))
    local_b = tuple(range(frames))

    wait_rows(0, local_f)
    conv_pair(0, w1v, 2, end0)
    for t in (1, 0):
        send_frame(1, t)
        send_rows(1, frames + t)
    pass_halo(0, 1)
    pass_halo(0, 0)
    wait_halo(0)
    conv_pair(0, w1v, 0, end0)
    for f in (HALO + 1, HALO):
        send_rows(1, f)
    turn_input(0, 0, frames + HALO)

    for t in range(step):
        loads[2 * step + 2 + t].wait()
        cross_copy(1, t).wait_recv()
    wait_rows(1, local_f)
    pass_halo(1, 1)
    conv_pair(1, w2v, 2, end1)
    for t in (2, 3):
        send_rows(2, t)

    def send_out(i, who):
        @pl.when(who)
        def _():
            for t in range(step):
                out_copy(i, t).start()

    send_out(0, first)
    pass_halo(1, 0)
    turn_input(1, HALO, frames)
    spread_delta(2, 2, 2)
    weight_grad(1, (2, 3), False, 1)
    wait_halo(1)
    conv_pair(1, w2v, 0, end1)
    for t in (0, 1):
        send_frame(2, t)
        send_rows(2, t)
    send_out(0, second)
    keep(0)
    turn_input(1, 0, HALO)
    spread_delta(2, 0, 2)
    weight_grad(1, (0, 1), True, 1)
    sum_phase_a(1)

    wait_rows(2, local_b)
    conv_pair(2, w2t, 0, end2)
    for t in (0, 1):
        send_frame(3, t)
        send_rows(3, t)
    sum_phase_b(1)
    pass_halo(2, 0)
    spread_delta(3, 0, 2)
    weight_grad(0, (0, 1), False, 0)
    pass_halo(2, 1)
    sum_phase_c(1, order[:2])
    wait_halo(2)
    conv_pair(2, w2t, 2, end2)
    for t in (2, 3):
        send_rows(3, t)
    sum_phase_c(1, order[2:])
    spread_delta(3, 2, 2)
    weight_grad(0, (2, 3), True, 0)
    sum_phase_a(0)
    total_phase_z(1)

    pass_halo(3, 0)
    pass_halo(3, 1)
    sum_phase_b(0)
    wait_rows(3, local_b)
    conv_pair(3, w1t, 0, end3)
    send_out(1, second)
    wait_halo(3)
    conv_pair(3, w1t, 2, end3)
    send_out(1, first)
    keep(1)
    total_phase_b(1)
    sum_phase_c(0, order)
    total_phase_z(0)
    total_phase_a(1)
    total_phase_b(0)
    total_phase_a(0)
    total_phase_end(1)
    total_phase_end(0)

    for i in range(2):
        for t in range(step):
            cross_copy(i, t).wait_send()
            out_copy(i, t).wait()
        a_copy(i).wait_send()
        for d in range(n_c):
            ga_copy(i, d).wait_send()
            for e in range(1, n_b):
                b_copy(i, d, e).wait_send()
                gb_copy(i, d, e).wait_send()
        for d in range(1, n_c):
            z_copy(i, d).wait_send()
            gz_copy(i, d).wait_send()
    for k in range(4):
        fwd = k < 2

        @pl.when(later if fwd else earlier)
        def _():
            for t in range(HALO):
                frame_copy(k, t).wait_send()

        @pl.when(jnp.logical_and(later if fwd else earlier, facing))
        def _():
            for t in range(HALO):
                corner_copy(k, t).wait_send()

        @pl.when(earlier if fwd else later)
        def _():
            for t in range(HALO):
                mate_copy(k, t).wait_send()
        for f in local_f if fwd else local_b:
            for way, there in ((0, below), (1, above)):
                @pl.when(there)
                def _():
                    row_copy(k, f, way).wait_send()


def finish(t1, t2, critic, clip_grad, g1, g2, critic_out, clip_grad_out, wide, g_sem, o_sem):
    copies = [
        pltpu.make_async_copy(src, dst, o_sem.at[i])
        for i, (src, dst) in enumerate(((critic, critic_out), (clip_grad, clip_grad_out)))
    ]
    for copy in copies:
        copy.start()
    part = wide.shape[1] // 3
    for i, (src, dst) in enumerate(((t1, g1), (t2, g2))):
        for a in range(3):
            at = pl.ds(a * part, part)
            wide[i, at] = src[at].astype(F32)
            copy = pltpu.make_async_copy(wide.at[i, at], dst.at[at], g_sem.at[i, a])
            copy.start()
            copies.append(copy)
    for copy in copies:
        copy.wait()


def on_device(n_frame, n_row, clip, first_kernel, second_kernel, cotangent):
    step, rows, width, ch = clip.shape
    grad_scale = 1.0 / float(step * n_frame * rows * n_row * width) ** 0.5
    n = n_frame * n_row
    frames, cw = 2 * step, width // 2 + MARGIN
    vmem, hbm = pl.BlockSpec(memory_space=pltpu.VMEM), pl.BlockSpec(memory_space=pltpu.HBM)
    weights = first_kernel.shape
    length = 27 * ch
    padded = -(-length // (16 * n)) * 16 * n
    counts = (2, n_row // 2, n_frame)
    size_a = padded // counts[0]
    piece = size_a // (counts[1] * counts[2])
    sems = pltpu.SemaphoreType.DMA
    block = (frames, rows, cw, ch)
    critic, clip_grad, t1, t2 = pl.pallas_call(
        functools.partial(kernel, n_frame, n_row, grad_scale),
        out_shape=(
            jax.ShapeDtypeStruct(clip.shape, BF16),
            jax.ShapeDtypeStruct(clip.shape, BF16),
            jax.ShapeDtypeStruct((padded, ch), BF16),
            jax.ShapeDtypeStruct((padded, ch), BF16),
        ),
        in_specs=[hbm] * 4,
        out_specs=(vmem,) * 4,
        scratch_shapes=[
            pltpu.VMEM((4, frames + HALO, rows + 2, cw, ch), BF16),
            pltpu.VMEM((step, rows, cw, ch), BF16),
            pltpu.VMEM(block, BF16),
            pltpu.VMEM(block, BF16),
            pltpu.VMEM(block, BF16),
            pltpu.VMEM(block, F32),
            pltpu.VMEM(weights, BF16),
            pltpu.VMEM(weights, BF16),
            pltpu.VMEM(weights, BF16),
            pltpu.VMEM(weights, BF16),
            pltpu.VMEM((2, frames + HALO, ch, (rows + 2) * (width // 2)), BF16),
            pltpu.VMEM((frames, rows, cw, 3 * ch), BF16),
            pltpu.VMEM((3, 3 * ch, 3 * ch), F32),
            pltpu.VMEM((2, padded, ch), BF16),
            pltpu.VMEM((2, size_a, ch), BF16),
            pltpu.VMEM((2, size_a, ch), BF16),
            pltpu.VMEM((2, counts[2], counts[1] - 1, piece, ch), BF16),
            pltpu.VMEM((2, counts[2] - 1, piece, ch), BF16),
            pltpu.VMEM((2, counts[2] - 1, piece, ch), BF16),
            sems((3 * step + 2,)),
            sems((2, step)), sems((2, step)),
            sems((2, step)), sems((2, step)),
            sems((4, HALO)), sems((4, HALO)),
            sems((4, HALO)), sems((4, HALO)),
            sems((4, frames + HALO, 2)), sems((4, frames + HALO, 2)),
            sems((2,)), sems((2,)),
            sems((2, counts[2], counts[1] - 1)), sems((2, counts[2], counts[1] - 1)),
            sems((2, counts[2] - 1)), sems((2, counts[2] - 1)),
            sems((2, counts[2])), sems((2, counts[2])),
            sems((2, counts[2], counts[1] - 1)), sems((2, counts[2], counts[1] - 1)),
            sems((2, counts[2] - 1)), sems((2, counts[2] - 1)),
        ],
        compiler_params=pltpu.CompilerParams(
            collective_id=0, has_side_effects=True, vmem_limit_bytes=32 * 2**20
        ),
    )(*(pltpu.with_memory_space_constraint(v, pltpu.HBM) for v in (clip, first_kernel, second_kernel, cotangent)))
    flat = jax.ShapeDtypeStruct((length, ch), F32)
    g1, g2, critic, clip_grad = pl.pallas_call(
        finish,
        out_shape=(flat, flat, jax.ShapeDtypeStruct(clip.shape, BF16), jax.ShapeDtypeStruct(clip.shape, BF16)),
        in_specs=[vmem] * 4,
        out_specs=(hbm,) * 4,
        scratch_shapes=[pltpu.VMEM((2, length, ch), F32), sems((2, 3)), sems((2,))],
        compiler_params=pltpu.CompilerParams(vmem_limit_bytes=16 * 2**20),
    )(t1, t2, critic, clip_grad)
    return critic, clip_grad, g1.reshape(weights), g2.reshape(weights)


def solution(mesh):
    placed = (P("frame", "row", None, None), P(), P(), P("frame", "row", None, None))
    return jax.shard_map(
        functools.partial(on_device, mesh.shape["frame"], mesh.shape["row"]),
        mesh=mesh,
        in_specs=placed,
        out_specs=(P("frame", "row", None, None), P("frame", "row", None, None), P(), P()),
        check_vma=False,
    )
```

```python
import functools

import jax
import jax.numpy as jnp
from jax import lax
from jax.experimental import pallas as pl
from jax.experimental.pallas import tpu as pltpu
from jax.sharding import PartitionSpec as P

MESH = pl.DeviceIdType.MESH
BF16, F32 = jnp.bfloat16, jnp.float32
MARGIN = 8
HALO = 2


def sum_groups(n_frame, n_row, me_f, me_r):
    pair, member = me_f // 2, lax.rem(me_f, 2)
    side, core = me_r // 2, lax.rem(me_r, 2)
    return (
        (2, core, lambda j: {"row": side * 2 + j}),
        (n_row // 2 * 2, side * 2 + member, lambda j: {"row": j // 2 * 2 + core, "frame": pair * 2 + lax.rem(j, 2)}),
        (n_frame // 2, pair, lambda j: {"frame": j * 2 + member}),
    )


def kernel(
    n_frame, n_row, grad_scale,
    clip, w1, w2, cot,
    critic, clip_grad, total1, total2,
    pads, cross, cotp, crit_s, cg_s, slope1, w1v, w2v, w1t, w2t, xt, d3, acc,
    mine, land_a, sum_a, land_b, sum_b, land_c,
    l_sem, x_send, x_recv, o_send, o_recv, f_send, f_recv, c_send, c_recv, r_send, r_recv,
    a_send, a_recv, b_send, b_recv, z_send, z_recv, ga_send, ga_recv, gb_send, gb_recv, gz_send, gz_recv,
):
    step, rows, width, ch = clip.shape
    half = width // 2
    cw = half + MARGIN
    frames = 2 * step
    me_f, me_r = lax.axis_index("frame"), lax.axis_index("row")
    member = lax.rem(me_f, 2)
    first, second = member == 0, member == 1
    later, earlier = me_f < n_frame - 2, me_f > 1
    below, above = me_r < n_row - 1, me_r > 0
    partner = {"frame": me_f + 1 - 2 * member}
    groups = sum_groups(n_frame, n_row, me_f, me_r)
    own = pl.multiple_of(member * MARGIN, MARGIN)
    odd = lax.rem(me_r, 2)
    facing = jnp.logical_or(jnp.logical_and(odd == 1, below), jnp.logical_and(odd == 0, above))
    mate, across = me_r + 1 - 2 * odd, me_r - 1 + 2 * odd

    def start_of(who):
        return pl.multiple_of(who * (half - MARGIN), MARGIN)

    barrier = pltpu.get_barrier_semaphore()
    for there, who in ((below, {"row": me_r + 1}), (above, {"row": me_r - 1})):
        @pl.when(there)
        def _():
            pl.semaphore_signal(barrier, inc=1, device_id=who, device_id_type=MESH)
    greeted = below.astype(jnp.int32) + above.astype(jnp.int32)
    for there, way in ((later, 2), (earlier, -2)):
        met = jnp.logical_and(there, facing)

        @pl.when(met)
        def _():
            who = {"frame": me_f + way, "row": across}
            pl.semaphore_signal(barrier, inc=1, device_id=who, device_id_type=MESH)
        greeted = greeted + met.astype(jnp.int32)
    for count, index, device in groups[1:]:
        for d in range(1, count):
            pl.semaphore_signal(barrier, inc=1, device_id=device(lax.rem(index + d, count)), device_id_type=MESH)
        greeted = greeted + (count - 1)

    loads = []
    for t in range(step):
        mine_at, other_at = pl.ds(start_of(member), cw), pl.ds(start_of(1 - member), cw)
        loads.append((clip.at[t, :, other_at], cross.at[t]))
        loads.append((clip.at[t, :, mine_at], pads.at[0, HALO + step * member + t, pl.ds(1, rows)]))
    loads.append((w1, w1v))
    loads.append((w2, w2v))
    for t in range(step):
        loads.append((cot.at[t, :, mine_at], cotp.at[step * member + t]))
    loads = [pltpu.make_async_copy(a, b, l_sem.at[i]) for i, (a, b) in enumerate(loads)]
    for load in loads:
        load.start()

    def zero(ref):
        ref[...] = jnp.zeros(ref.shape, ref.dtype)

    for k in range(4):
        @pl.when(jnp.logical_not(earlier if k < 2 else later))
        def _():
            for f in ((0, 1) if k < 2 else (frames, frames + 1)):
                zero(pads.at[k, f])

        @pl.when(jnp.logical_not(above))
        def _():
            for f in range(frames + HALO):
                zero(pads.at[k, f, 0])

        @pl.when(jnp.logical_not(below))
        def _():
            for f in range(frames + HALO):
                zero(pads.at[k, f, rows + 1])
    used = 27 * ch
    for i in range(2):
        mine[i, pl.ds(used, mine.shape[1] - used)] = jnp.zeros((mine.shape[1] - used, ch), BF16)

    pl.semaphore_wait(barrier, greeted)

    def remote(src, dst, send, recv, who):
        return pltpu.make_async_remote_copy(
            src_ref=src, dst_ref=dst, send_sem=send, recv_sem=recv, device_id=who, device_id_type=MESH
        )

    def cross_copy(i, t):
        if i == 0:
            src, dst = cross.at[t], pads.at[0, HALO + step * member + t, pl.ds(1, rows)]
        else:
            src, dst = cot.at[t, :, pl.ds(start_of(1 - member), cw)], cotp.at[step * member + t]
        return remote(src, dst, x_send.at[i, t], x_recv.at[i, t], partner)

    def out_copy(i, t):
        src, dst = ((crit_s, critic), (cg_s, clip_grad))[i]
        return remote(
            src.at[step * (1 - member) + t, :, pl.ds(own, half)],
            dst.at[t, :, pl.ds(pl.multiple_of(member * half, half), half)],
            o_send.at[i, t], o_recv.at[i, t], partner,
        )

    def keep(i):
        src, dst = ((crit_s, critic), (cg_s, clip_grad))[i]
        for t in range(step):
            dst[t, :, pl.ds(pl.multiple_of(member * half, half), half)] = src[step * member + t, :, pl.ds(own, half)]

    def frame_copy(k, t):
        fwd = k < 2
        src, dst = (frames + t, t) if fwd else (t, frames + t)
        return remote(
            pads.at[k, src, pl.ds(1, rows)], pads.at[k, dst, pl.ds(1, rows)],
            f_send.at[k, t], f_recv.at[k, t], {"frame": me_f + 2 if fwd else me_f - 2},
        )

    def row_copy(k, f, way):
        src, dst = ((rows, 0), (1, rows + 1))[way]
        return remote(
            pads.at[k, f, src], pads.at[k, f, dst],
            r_send.at[k, f, way], r_recv.at[k, f, way], {"row": me_r + 1 if way == 0 else me_r - 1},
        )

    def send_rows(k, f):
        @pl.when(below)
        def _():
            row_copy(k, f, 0).start()

        @pl.when(above)
        def _():
            row_copy(k, f, 1).start()

    def wait_rows(k, fs):
        for f in fs:
            @pl.when(above)
            def _():
                row_copy(k, f, 0).wait_recv()

            @pl.when(below)
            def _():
                row_copy(k, f, 1).wait_recv()

    def corner_copy(k, t):
        fwd = k < 2
        src, dst = (frames + t, t) if fwd else (t, frames + t)
        return remote(
            pads.at[k, src, 1 + odd * (rows - 1)], pads.at[k, dst, (1 - odd) * (rows + 1)],
            c_send.at[k, t], c_recv.at[k, t], {"frame": me_f + 2 if fwd else me_f - 2, "row": across},
        )

    def mate_copy(k, t):
        f = t if k < 2 else frames + t
        return remote(
            pads.at[k, f, rows - odd * (rows - 1)], pads.at[k, f, odd * (rows + 1)],
            r_send.at[k, f, 0], r_recv.at[k, f, 0], {"row": mate},
        )

    def send_frame(k, t):
        there = later if k < 2 else earlier

        @pl.when(there)
        def _():
            frame_copy(k, t).start()

        @pl.when(jnp.logical_and(there, facing))
        def _():
            corner_copy(k, t).start()

    def pass_halo(k, t):
        @pl.when(earlier if k < 2 else later)
        def _():
            frame_copy(k, t).wait_recv()
            mate_copy(k, t).start()

    def wait_halo(k):
        there = earlier if k < 2 else later

        @pl.when(there)
        def _():
            for t in range(HALO):
                mate_copy(k, t).wait_recv()

        @pl.when(jnp.logical_and(there, facing))
        def _():
            for t in range(HALO):
                corner_copy(k, t).wait_recv()

    (_, core, to_core), (n_b, in_b, to_b), (n_c, in_c, to_c) = groups
    half_rows = sum_a.shape[1]
    piece = half_rows // (n_b * n_c)

    def aligned(x):
        return pl.multiple_of(x, 16)

    def block(q):
        return aligned(q * (n_b * piece))

    def a_copy(i):
        src = mine.at[i, pl.ds(aligned((1 - core) * half_rows), half_rows)]
        return remote(src, land_a.at[i], a_send.at[i], a_recv.at[i], to_core(1 - core))

    def b_copy(i, d, e):
        peer = lax.rem(in_b + e, n_b)
        src = sum_a.at[i, pl.ds(aligned(block(lax.rem(in_c + d, n_c)) + peer * piece), piece)]
        return remote(src, land_b.at[i, d, e - 1], b_send.at[i, d, e - 1], b_recv.at[i, d, e - 1], to_b(peer))

    def z_copy(i, d):
        peer = lax.rem(in_c + d, n_c)
        return remote(sum_b.at[i, d - 1], land_c.at[i, d - 1], z_send.at[i, d - 1], z_recv.at[i, d - 1], to_c(peer))

    near = sorted(range(1, n_c), key=lambda d: min(d, n_c - d))
    order = tuple(reversed(near))

    def sum_phase_a(i):
        a_copy(i).start()

    def sum_phase_b(i):
        a_copy(i).wait_recv()
        kept = mine[i, pl.ds(aligned(core * half_rows), half_rows)].astype(F32)
        sum_a[i] = (kept + land_a[i].astype(F32)).astype(BF16)
        for d in order + (0,):
            for e in range(1, n_b):
                b_copy(i, d, e).start()

    def plane_sum(i, d):
        for e in range(1, n_b):
            b_copy(i, d, e).wait_recv()
        z = sum_a[i, pl.ds(aligned(block(lax.rem(in_c + d, n_c)) + in_b * piece), piece)].astype(F32)
        for e in range(1, n_b):
            z = z + land_b[i, d, e - 1].astype(F32)
        return z

    def sum_phase_c(i, ds):
        for d in ds:
            sum_b[i, d - 1] = plane_sum(i, d).astype(BF16)
            z_copy(i, d).start()

    def total_at(i, q, j, n):
        lo = aligned(core * half_rows + block(q) + j * piece)
        return (total1, total2)[i].at[pl.ds(lo, n)]

    def gz_copy(i, d):
        part = total_at(i, in_c, in_b, piece)
        return remote(part, part, gz_send.at[i, d - 1], gz_recv.at[i, d - 1], to_c(lax.rem(in_c + d, n_c)))

    def source(d):
        return lax.rem(in_c + n_c - d, n_c)

    def gb_copy(i, d, e):
        part = total_at(i, source(d), in_b, piece)
        return remote(
            part, part, gb_send.at[i, d, e - 1], gb_recv.at[i, d, e - 1], to_b(lax.rem(in_b + e, n_b))
        )

    def ga_copy(i, d):
        part = total_at(i, source(d), 0, n_b * piece)
        return remote(part, part, ga_send.at[i, d], ga_recv.at[i, d], to_core(1 - core))

    def gx_copy(d):
        part = total_at(1, source(d), in_b, piece)
        return remote(part, part, gb_send.at[1, d, 0], gb_recv.at[1, d, 0], partner)

    def gy_copy(d):
        side = me_r // 2
        part = total_at(1, source(d), side * 2, 2 * piece)
        return remote(part, part, gb_send.at[1, d, 1], gb_recv.at[1, d, 1], {"row": me_r + 2 - 4 * side})

    def total_phase_x():
        for d in near:
            gz_copy(1, d).wait_recv()
            gx_copy(d).start()

    def total_phase_y(ds):
        for d in ds:
            gx_copy(d).wait_recv()
            gy_copy(d).start()

    def total_phase_z(i):
        z = plane_sum(i, 0)
        for d in range(1, n_c):
            z_copy(i, d).wait_recv()
            z = z + land_c[i, d - 1].astype(F32)
        total_at(i, in_c, in_b, piece)[...] = z.astype(BF16)
        for d in order:
            gz_copy(i, d).start()
        if i == 1:
            gx_copy(0).start()
        else:
            for e in range(1, n_b):
                gb_copy(i, 0, e).start()

    def total_phase_b(i):
        for d in near:
            gz_copy(i, d).wait_recv()
            for e in range(1, n_b):
                gb_copy(i, d, e).start()

    def total_phase_a(i):
        for d in [0] + near:
            if i == 1:
                gy_copy(d).wait_recv()
            else:
                for e in range(1, n_b):
                    gb_copy(i, d, e).wait_recv()
            ga_copy(i, d).start()

    def total_phase_end(i):
        for d in range(n_c):
            ga_copy(i, d).wait_recv()

    def shifted(p):
        left, mid, right = (p[:, c * ch : (c + 1) * ch].reshape(rows, cw, ch) for c in range(3))
        pos = lax.broadcasted_iota(jnp.int32, (rows, cw, ch), 1)
        return (
            jnp.where(pos == 0, 0.0, pltpu.roll(left, 1, 1)) + mid
            + jnp.where(pos == cw - 1, 0.0, pltpu.roll(right, cw - 1, 1))
        )

    def conv_pair(k, w, t, epilogue):
        def x(j, b):
            return pads[k, t + j, pl.ds(b, rows)].reshape(rows * cw, ch)

        def taps(a, b):
            return jnp.concatenate([w[a, b, c] for c in range(3)], axis=1)

        def both(j, b):
            return jnp.concatenate([taps(j, b), taps(j - 1, b)], axis=1)

        def dot(xs, ws):
            return jnp.dot(
                jnp.concatenate(xs, axis=1), jnp.concatenate(ws, axis=0), preferred_element_type=F32
            )

        mid = [(j, b) for j in (1, 2) for b in range(3)]
        p = dot([x(j, b) for j, b in mid], [both(j, b) for j, b in mid])
        q0 = dot([x(0, b) for b in range(3)], [taps(0, b) for b in range(3)])
        q1 = dot([x(3, b) for b in range(3)], [taps(2, b) for b in range(3)])
        epilogue(t, shifted(p[:, : 3 * ch] + q0))
        epilogue(t + 1, shifted(p[:, 3 * ch :] + q1))

    inner = pl.ds(1, rows)

    def end0(t, z):
        sigma = jax.nn.sigmoid(z)
        slope1[t] = sigma * (1.0 + z * (1.0 - sigma))
        pads[1, HALO + t, inner] = (z * sigma).astype(BF16)

    def end1(t, z):
        sigma = jax.nn.sigmoid(z)
        crit_s[t] = (z * sigma).astype(BF16)
        delta = cotp[t].astype(F32) * (sigma * (1.0 + z * (1.0 - sigma)))
        pads[2, t, inner] = delta.astype(BF16)

    def end2(t, z):
        pads[3, t, inner] = (z * slope1[t]).astype(BF16)

    def end3(t, z):
        cg_s[t] = z.astype(BF16)

    def turn_weights():
        def one(i, c):
            a, b = i // 3, lax.rem(i, 3)
            for src, dst in ((w1v, w1t), (w2v, w2t)):
                for q in range(3):
                    dst[a, b, q] = src[2 - a, 2 - b, 2 - q].T
            return c
        lax.fori_loop(0, 9, one, 0)

    def turn_input(k, lo, n):
        def one(f, c):
            for r in range(rows + 2):
                xt[k, f, :, r * half : (r + 1) * half] = pads[k, f, r, pl.ds(own, half)].T
            return c
        lax.fori_loop(lo, lo + n, one, 0)

    def spread_delta(k, lo, n):
        def one(t, c):
            pos = lax.broadcasted_iota(jnp.int32, (cw, ch), 0)
            for r in range(rows):
                x = pads[k, t, r + 1].astype(F32)
                d3[t, r, :, 0:ch] = jnp.where(pos == cw - 1, 0.0, pltpu.roll(x, cw - 1, 0)).astype(BF16)
                d3[t, r, :, ch : 2 * ch] = pads[k, t, r + 1]
                d3[t, r, :, 2 * ch :] = jnp.where(pos == 0, 0.0, pltpu.roll(x, 1, 0)).astype(BF16)
            return c
        lax.fori_loop(lo, lo + n, one, 0)

    def weight_grad(k, ts, last, i):
        def one(a, c):
            z = None
            for t in ts:
                x = xt[k, t + a]
                left = jnp.concatenate([x[:, b * half : (b + rows) * half] for b in range(3)], axis=0)
                right = d3[t, :, pl.ds(own, half)].reshape(rows * half, 3 * ch)
                p = jnp.dot(left, right, preferred_element_type=F32)
                z = p if z is None else z + p
            if not last:
                acc[a] = z
            else:
                z = (z + acc[a]) * grad_scale
                for b in range(3):
                    for q in range(3):
                        at = pl.multiple_of(a * (9 * ch) + (b * 3 + q) * ch, ch)
                        mine[i, pl.ds(at, ch)] = z[b * ch : (b + 1) * ch, q * ch : (q + 1) * ch].astype(BF16)
            return c
        lax.fori_loop(0, 3, one, 0)

    for t in range(step):
        loads[2 * t].wait()
    for t in (1, 0):
        cross_copy(0, t).start()
    for t in range(step):
        loads[2 * t + 1].wait()

    def publish_clip(who, fs):
        @pl.when(who)
        def _():
            for f in fs:
                if f >= frames:
                    send_frame(0, f - frames)
                send_rows(0, f)

    publish_clip(second, (frames + 1, frames))
    publish_clip(first, (HALO + 1, HALO))
    for t in (1, 0):
        cross_copy(1, t).start()
    loads[2 * step].wait()
    loads[2 * step + 1].wait()
    turn_weights()
    for t in (1, 0):
        cross_copy(0, t).wait_recv()
        publish_clip(first, (HALO + step + t,))
        publish_clip(second, (HALO + t,))

    local_f = tuple(range(HALO, HALO + frames))
    local_b = tuple(range(frames))

    wait_rows(0, local_f)
    conv_pair(0, w1v, 2, end0)
    for t in (1, 0):
        send_frame(1, t)
        send_rows(1, frames + t)
    pass_halo(0, 1)
    pass_halo(0, 0)
    wait_halo(0)
    conv_pair(0, w1v, 0, end0)
    for f in (HALO + 1, HALO):
        send_rows(1, f)
    turn_input(0, 0, frames + HALO)

    for t in range(step):
        loads[2 * step + 2 + t].wait()
        cross_copy(1, t).wait_recv()
    wait_rows(1, local_f)
    pass_halo(1, 1)
    conv_pair(1, w2v, 2, end1)
    for t in (2, 3):
        send_rows(2, t)

    def send_out(i, who):
        @pl.when(who)
        def _():
            for t in range(step):
                out_copy(i, t).start()

    send_out(0, first)
    pass_halo(1, 0)
    turn_input(1, HALO, frames)
    spread_delta(2, 2, 2)
    weight_grad(1, (2, 3), False, 1)
    wait_halo(1)
    conv_pair(1, w2v, 0, end1)
    for t in (0, 1):
        send_frame(2, t)
        send_rows(2, t)
    send_out(0, second)
    keep(0)
    turn_input(1, 0, HALO)
    spread_delta(2, 0, 2)
    weight_grad(1, (0, 1), True, 1)
    sum_phase_a(1)

    wait_rows(2, local_b)
    conv_pair(2, w2t, 0, end2)
    for t in (0, 1):
        send_frame(3, t)
        send_rows(3, t)
    sum_phase_b(1)
    pass_halo(2, 0)
    spread_delta(3, 0, 2)
    weight_grad(0, (0, 1), False, 0)
    pass_halo(2, 1)
    sum_phase_c(1, order[:2])
    wait_halo(2)
    conv_pair(2, w2t, 2, end2)
    for t in (2, 3):
        send_rows(3, t)
    sum_phase_c(1, order[2:])
    spread_delta(3, 2, 2)
    weight_grad(0, (2, 3), True, 0)
    sum_phase_a(0)

    pass_halo(3, 0)
    pass_halo(3, 1)
    wait_rows(3, local_b)
    conv_pair(3, w1t, 0, end3)
    sum_phase_b(0)
    total_phase_z(1)
    wait_halo(3)
    conv_pair(3, w1t, 2, end3)
    keep(1)
    sum_phase_c(0, order[:1])
    total_phase_x()
    send_out(1, second)
    send_out(1, first)
    sum_phase_c(0, order[1:])
    total_phase_y([0] + near[:1])
    total_phase_z(0)
    total_phase_y(near[1:])
    total_phase_b(0)
    total_phase_a(1)
    total_phase_a(0)
    total_phase_end(1)
    total_phase_end(0)

    for i in range(2):
        for t in range(step):
            cross_copy(i, t).wait_send()
            out_copy(i, t).wait()
        a_copy(i).wait_send()
        for d in range(n_c):
            ga_copy(i, d).wait_send()
            for e in range(1, n_b):
                b_copy(i, d, e).wait_send()
            if i == 1:
                gx_copy(d).wait_send()
                gy_copy(d).wait_send()
            else:
                for e in range(1, n_b):
                    gb_copy(i, d, e).wait_send()
        for d in range(1, n_c):
            z_copy(i, d).wait_send()
            gz_copy(i, d).wait_send()
    for k in range(4):
        fwd = k < 2

        @pl.when(later if fwd else earlier)
        def _():
            for t in range(HALO):
                frame_copy(k, t).wait_send()

        @pl.when(jnp.logical_and(later if fwd else earlier, facing))
        def _():
            for t in range(HALO):
                corner_copy(k, t).wait_send()

        @pl.when(earlier if fwd else later)
        def _():
            for t in range(HALO):
                mate_copy(k, t).wait_send()
        for f in local_f if fwd else local_b:
            for way, there in ((0, below), (1, above)):
                @pl.when(there)
                def _():
                    row_copy(k, f, way).wait_send()


def finish(t1, t2, critic, clip_grad, g1, g2, critic_out, clip_grad_out, wide, g_sem, o_sem):
    copies = [
        pltpu.make_async_copy(src, dst, o_sem.at[i])
        for i, (src, dst) in enumerate(((critic, critic_out), (clip_grad, clip_grad_out)))
    ]
    for copy in copies:
        copy.start()
    part = wide.shape[1] // 3
    for i, (src, dst) in enumerate(((t1, g1), (t2, g2))):
        for a in range(3):
            at = pl.ds(a * part, part)
            wide[i, at] = src[at].astype(F32)
            copy = pltpu.make_async_copy(wide.at[i, at], dst.at[at], g_sem.at[i, a])
            copy.start()
            copies.append(copy)
    for copy in copies:
        copy.wait()


def on_device(n_frame, n_row, clip, first_kernel, second_kernel, cotangent):
    step, rows, width, ch = clip.shape
    grad_scale = 1.0 / float(step * n_frame * rows * n_row * width) ** 0.5
    n = n_frame * n_row
    frames, cw = 2 * step, width // 2 + MARGIN
    vmem, hbm = pl.BlockSpec(memory_space=pltpu.VMEM), pl.BlockSpec(memory_space=pltpu.HBM)
    weights = first_kernel.shape
    length = 27 * ch
    padded = -(-length // (16 * n)) * 16 * n
    counts = (2, n_row // 2 * 2, n_frame // 2)
    size_a = padded // counts[0]
    piece = size_a // (counts[1] * counts[2])
    sems = pltpu.SemaphoreType.DMA
    block = (frames, rows, cw, ch)
    critic, clip_grad, t1, t2 = pl.pallas_call(
        functools.partial(kernel, n_frame, n_row, grad_scale),
        out_shape=(
            jax.ShapeDtypeStruct(clip.shape, BF16),
            jax.ShapeDtypeStruct(clip.shape, BF16),
            jax.ShapeDtypeStruct((padded, ch), BF16),
            jax.ShapeDtypeStruct((padded, ch), BF16),
        ),
        in_specs=[hbm] * 4,
        out_specs=(vmem,) * 4,
        scratch_shapes=[
            pltpu.VMEM((4, frames + HALO, rows + 2, cw, ch), BF16),
            pltpu.VMEM((step, rows, cw, ch), BF16),
            pltpu.VMEM(block, BF16),
            pltpu.VMEM(block, BF16),
            pltpu.VMEM(block, BF16),
            pltpu.VMEM(block, F32),
            pltpu.VMEM(weights, BF16),
            pltpu.VMEM(weights, BF16),
            pltpu.VMEM(weights, BF16),
            pltpu.VMEM(weights, BF16),
            pltpu.VMEM((2, frames + HALO, ch, (rows + 2) * (width // 2)), BF16),
            pltpu.VMEM((frames, rows, cw, 3 * ch), BF16),
            pltpu.VMEM((3, 3 * ch, 3 * ch), F32),
            pltpu.VMEM((2, padded, ch), BF16),
            pltpu.VMEM((2, size_a, ch), BF16),
            pltpu.VMEM((2, size_a, ch), BF16),
            pltpu.VMEM((2, counts[2], counts[1] - 1, piece, ch), BF16),
            pltpu.VMEM((2, counts[2] - 1, piece, ch), BF16),
            pltpu.VMEM((2, counts[2] - 1, piece, ch), BF16),
            sems((3 * step + 2,)),
            sems((2, step)), sems((2, step)),
            sems((2, step)), sems((2, step)),
            sems((4, HALO)), sems((4, HALO)),
            sems((4, HALO)), sems((4, HALO)),
            sems((4, frames + HALO, 2)), sems((4, frames + HALO, 2)),
            sems((2,)), sems((2,)),
            sems((2, counts[2], counts[1] - 1)), sems((2, counts[2], counts[1] - 1)),
            sems((2, counts[2] - 1)), sems((2, counts[2] - 1)),
            sems((2, counts[2])), sems((2, counts[2])),
            sems((2, counts[2], counts[1] - 1)), sems((2, counts[2], counts[1] - 1)),
            sems((2, counts[2] - 1)), sems((2, counts[2] - 1)),
        ],
        compiler_params=pltpu.CompilerParams(
            collective_id=0, has_side_effects=True, vmem_limit_bytes=32 * 2**20
        ),
    )(*(pltpu.with_memory_space_constraint(v, pltpu.HBM) for v in (clip, first_kernel, second_kernel, cotangent)))
    flat = jax.ShapeDtypeStruct((length, ch), F32)
    g1, g2, critic, clip_grad = pl.pallas_call(
        finish,
        out_shape=(flat, flat, jax.ShapeDtypeStruct(clip.shape, BF16), jax.ShapeDtypeStruct(clip.shape, BF16)),
        in_specs=[vmem] * 4,
        out_specs=(hbm,) * 4,
        scratch_shapes=[pltpu.VMEM((2, length, ch), F32), sems((2, 3)), sems((2,))],
        compiler_params=pltpu.CompilerParams(vmem_limit_bytes=16 * 2**20),
    )(t1, t2, critic, clip_grad)
    return critic, clip_grad, g1.reshape(weights), g2.reshape(weights)


def solution(mesh):
    placed = (P("frame", "row", None, None), P(), P(), P("frame", "row", None, None))
    return jax.shard_map(
        functools.partial(on_device, mesh.shape["frame"], mesh.shape["row"]),
        mesh=mesh,
        in_specs=placed,
        out_specs=(P("frame", "row", None, None), P("frame", "row", None, None), P(), P()),
        check_vma=False,
    )
```

```python
import functools

import jax
import jax.numpy as jnp
from jax import lax
from jax.experimental import pallas as pl
from jax.experimental.pallas import tpu as pltpu
from jax.sharding import PartitionSpec as P

MESH = pl.DeviceIdType.MESH
BF16, F32 = jnp.bfloat16, jnp.float32
MARGIN = 8
HALO = 2


def sum_groups(n_frame, n_row, me_f, me_r):
    pair, member = me_f // 2, lax.rem(me_f, 2)
    side, core = me_r // 2, lax.rem(me_r, 2)
    return (
        (2, core, lambda j: {"row": side * 2 + j}),
        (n_row // 2 * 2, side * 2 + member, lambda j: {"row": j // 2 * 2 + core, "frame": pair * 2 + lax.rem(j, 2)}),
        (n_frame // 2, pair, lambda j: {"frame": j * 2 + member}),
    )


def kernel(
    n_frame, n_row, grad_scale,
    clip, w1, w2, cot,
    critic, clip_grad, total1, total2,
    pads, cross, cotp, crit_s, cg_s, slope1, w1v, w2v, w1t, w2t, xt, d3, acc,
    mine, land_a, sum_a, land_b, sum_b, land_c,
    l_sem, x_send, x_recv, o_send, o_recv, f_send, f_recv, c_send, c_recv, r_send, r_recv,
    a_send, a_recv, b_send, b_recv, z_send, z_recv, ga_send, ga_recv, gb_send, gb_recv, gz_send, gz_recv,
):
    step, rows, width, ch = clip.shape
    half = width // 2
    cw = half + MARGIN
    frames = 2 * step
    me_f, me_r = lax.axis_index("frame"), lax.axis_index("row")
    member = lax.rem(me_f, 2)
    first, second = member == 0, member == 1
    later, earlier = me_f < n_frame - 2, me_f > 1
    below, above = me_r < n_row - 1, me_r > 0
    partner = {"frame": me_f + 1 - 2 * member}
    groups = sum_groups(n_frame, n_row, me_f, me_r)
    own = pl.multiple_of(member * MARGIN, MARGIN)
    odd = lax.rem(me_r, 2)
    facing = jnp.logical_or(jnp.logical_and(odd == 1, below), jnp.logical_and(odd == 0, above))
    mate, across = me_r + 1 - 2 * odd, me_r - 1 + 2 * odd

    def start_of(who):
        return pl.multiple_of(who * (half - MARGIN), MARGIN)

    barrier = pltpu.get_barrier_semaphore()
    for there, who in ((below, {"row": me_r + 1}), (above, {"row": me_r - 1})):
        @pl.when(there)
        def _():
            pl.semaphore_signal(barrier, inc=1, device_id=who, device_id_type=MESH)
    greeted = below.astype(jnp.int32) + above.astype(jnp.int32)
    for there, way in ((later, 2), (earlier, -2)):
        met = jnp.logical_and(there, facing)

        @pl.when(met)
        def _():
            who = {"frame": me_f + way, "row": across}
            pl.semaphore_signal(barrier, inc=1, device_id=who, device_id_type=MESH)
        greeted = greeted + met.astype(jnp.int32)
    for count, index, device in groups[1:]:
        for d in range(1, count):
            pl.semaphore_signal(barrier, inc=1, device_id=device(lax.rem(index + d, count)), device_id_type=MESH)
        greeted = greeted + (count - 1)

    loads = []
    for t in range(step):
        mine_at, other_at = pl.ds(start_of(member), cw), pl.ds(start_of(1 - member), cw)
        loads.append((clip.at[t, :, other_at], cross.at[t]))
        loads.append((clip.at[t, :, mine_at], pads.at[0, HALO + step * member + t, pl.ds(1, rows)]))
    loads.append((w1, w1v))
    loads.append((w2, w2v))
    for t in range(step):
        loads.append((cot.at[t, :, mine_at], cotp.at[step * member + t]))
    loads = [pltpu.make_async_copy(a, b, l_sem.at[i]) for i, (a, b) in enumerate(loads)]
    for load in loads:
        load.start()

    def zero(ref):
        ref[...] = jnp.zeros(ref.shape, ref.dtype)

    for k in range(4):
        @pl.when(jnp.logical_not(earlier if k < 2 else later))
        def _():
            for f in ((0, 1) if k < 2 else (frames, frames + 1)):
                zero(pads.at[k, f])

        @pl.when(jnp.logical_not(above))
        def _():
            for f in range(frames + HALO):
                zero(pads.at[k, f, 0])

        @pl.when(jnp.logical_not(below))
        def _():
            for f in range(frames + HALO):
                zero(pads.at[k, f, rows + 1])
    used = 27 * ch
    for i in range(2):
        mine[i, pl.ds(used, mine.shape[1] - used)] = jnp.zeros((mine.shape[1] - used, ch), BF16)

    pl.semaphore_wait(barrier, greeted)

    def remote(src, dst, send, recv, who):
        return pltpu.make_async_remote_copy(
            src_ref=src, dst_ref=dst, send_sem=send, recv_sem=recv, device_id=who, device_id_type=MESH
        )

    def cross_copy(i, t):
        if i == 0:
            src, dst = cross.at[t], pads.at[0, HALO + step * member + t, pl.ds(1, rows)]
        else:
            src, dst = cot.at[t, :, pl.ds(start_of(1 - member), cw)], cotp.at[step * member + t]
        return remote(src, dst, x_send.at[i, t], x_recv.at[i, t], partner)

    def out_copy(i, t):
        src, dst = ((crit_s, critic), (cg_s, clip_grad))[i]
        return remote(
            src.at[step * (1 - member) + t, :, pl.ds(own, half)],
            dst.at[t, :, pl.ds(pl.multiple_of(member * half, half), half)],
            o_send.at[i, t], o_recv.at[i, t], partner,
        )

    def keep(i):
        src, dst = ((crit_s, critic), (cg_s, clip_grad))[i]
        for t in range(step):
            dst[t, :, pl.ds(pl.multiple_of(member * half, half), half)] = src[step * member + t, :, pl.ds(own, half)]

    def frame_copy(k, t):
        fwd = k < 2
        src, dst = (frames + t, t) if fwd else (t, frames + t)
        return remote(
            pads.at[k, src, pl.ds(1, rows)], pads.at[k, dst, pl.ds(1, rows)],
            f_send.at[k, t], f_recv.at[k, t], {"frame": me_f + 2 if fwd else me_f - 2},
        )

    def row_copy(k, f, way):
        src, dst = ((rows, 0), (1, rows + 1))[way]
        return remote(
            pads.at[k, f, src], pads.at[k, f, dst],
            r_send.at[k, f, way], r_recv.at[k, f, way], {"row": me_r + 1 if way == 0 else me_r - 1},
        )

    def send_rows(k, f):
        @pl.when(below)
        def _():
            row_copy(k, f, 0).start()

        @pl.when(above)
        def _():
            row_copy(k, f, 1).start()

    def wait_rows(k, fs):
        for f in fs:
            @pl.when(above)
            def _():
                row_copy(k, f, 0).wait_recv()

            @pl.when(below)
            def _():
                row_copy(k, f, 1).wait_recv()

    def corner_copy(k, t):
        fwd = k < 2
        src, dst = (frames + t, t) if fwd else (t, frames + t)
        return remote(
            pads.at[k, src, 1 + odd * (rows - 1)], pads.at[k, dst, (1 - odd) * (rows + 1)],
            c_send.at[k, t], c_recv.at[k, t], {"frame": me_f + 2 if fwd else me_f - 2, "row": across},
        )

    def mate_copy(k, t):
        f = t if k < 2 else frames + t
        return remote(
            pads.at[k, f, rows - odd * (rows - 1)], pads.at[k, f, odd * (rows + 1)],
            r_send.at[k, f, 0], r_recv.at[k, f, 0], {"row": mate},
        )

    def send_frame(k, t):
        there = later if k < 2 else earlier

        @pl.when(there)
        def _():
            frame_copy(k, t).start()

        @pl.when(jnp.logical_and(there, facing))
        def _():
            corner_copy(k, t).start()

    def pass_halo(k, t):
        @pl.when(earlier if k < 2 else later)
        def _():
            frame_copy(k, t).wait_recv()
            mate_copy(k, t).start()

    def wait_halo(k):
        there = earlier if k < 2 else later

        @pl.when(there)
        def _():
            for t in range(HALO):
                mate_copy(k, t).wait_recv()

        @pl.when(jnp.logical_and(there, facing))
        def _():
            for t in range(HALO):
                corner_copy(k, t).wait_recv()

    (_, core, to_core), (n_b, in_b, to_b), (n_c, in_c, to_c) = groups
    half_rows = sum_a.shape[1]
    piece = half_rows // (n_b * n_c)

    def aligned(x):
        return pl.multiple_of(x, 16)

    def block(q):
        return aligned(q * (n_b * piece))

    def a_copy(i):
        src = mine.at[i, pl.ds(aligned((1 - core) * half_rows), half_rows)]
        return remote(src, land_a.at[i], a_send.at[i], a_recv.at[i], to_core(1 - core))

    def b_copy(i, d, e):
        peer = lax.rem(in_b + e, n_b)
        src = sum_a.at[i, pl.ds(aligned(block(lax.rem(in_c + d, n_c)) + peer * piece), piece)]
        return remote(src, land_b.at[i, d, e - 1], b_send.at[i, d, e - 1], b_recv.at[i, d, e - 1], to_b(peer))

    def z_copy(i, d):
        peer = lax.rem(in_c + d, n_c)
        return remote(sum_b.at[i, d - 1], land_c.at[i, d - 1], z_send.at[i, d - 1], z_recv.at[i, d - 1], to_c(peer))

    near = sorted(range(1, n_c), key=lambda d: min(d, n_c - d))
    order = tuple(reversed(near))

    def sum_phase_a(i):
        a_copy(i).start()

    def sum_phase_b(i):
        a_copy(i).wait_recv()
        kept = mine[i, pl.ds(aligned(core * half_rows), half_rows)].astype(F32)
        sum_a[i] = (kept + land_a[i].astype(F32)).astype(BF16)
        for d in order + (0,):
            for e in range(1, n_b):
                b_copy(i, d, e).start()

    def plane_sum(i, d):
        for e in range(1, n_b):
            b_copy(i, d, e).wait_recv()
        z = sum_a[i, pl.ds(aligned(block(lax.rem(in_c + d, n_c)) + in_b * piece), piece)].astype(F32)
        for e in range(1, n_b):
            z = z + land_b[i, d, e - 1].astype(F32)
        return z

    def sum_phase_c(i, ds):
        for d in ds:
            sum_b[i, d - 1] = plane_sum(i, d).astype(BF16)
            z_copy(i, d).start()

    def total_at(i, q, j, n):
        lo = aligned(core * half_rows + block(q) + j * piece)
        return (total1, total2)[i].at[pl.ds(lo, n)]

    def gz_copy(i, d):
        part = total_at(i, in_c, in_b, piece)
        return remote(part, part, gz_send.at[i, d - 1], gz_recv.at[i, d - 1], to_c(lax.rem(in_c + d, n_c)))

    def source(d):
        return lax.rem(in_c + n_c - d, n_c)

    def gb_copy(i, d, e):
        part = total_at(i, source(d), in_b, piece)
        return remote(
            part, part, gb_send.at[i, d, e - 1], gb_recv.at[i, d, e - 1], to_b(lax.rem(in_b + e, n_b))
        )

    def ga_copy(i, d):
        part = total_at(i, source(d), 0, n_b * piece)
        return remote(part, part, ga_send.at[i, d], ga_recv.at[i, d], to_core(1 - core))

    def gx_copy(d):
        part = total_at(1, source(d), in_b, piece)
        return remote(part, part, gb_send.at[1, d, 0], gb_recv.at[1, d, 0], partner)

    def gy_copy(d):
        side = me_r // 2
        part = total_at(1, source(d), side * 2, 2 * piece)
        return remote(part, part, gb_send.at[1, d, 1], gb_recv.at[1, d, 1], {"row": me_r + 2 - 4 * side})

    def total_phase_x():
        for d in near:
            gz_copy(1, d).wait_recv()
            gx_copy(d).start()

    def total_phase_y(ds):
        for d in ds:
            gx_copy(d).wait_recv()
            gy_copy(d).start()

    def total_phase_z(i):
        z = plane_sum(i, 0)
        for d in range(1, n_c):
            z_copy(i, d).wait_recv()
            z = z + land_c[i, d - 1].astype(F32)
        total_at(i, in_c, in_b, piece)[...] = z.astype(BF16)
        for d in order:
            gz_copy(i, d).start()
        if i == 1:
            gx_copy(0).start()
        else:
            for e in range(1, n_b):
                gb_copy(i, 0, e).start()

    def total_phase_b(i):
        for d in near:
            gz_copy(i, d).wait_recv()
            for e in range(1, n_b):
                gb_copy(i, d, e).start()

    def total_phase_a(i):
        for d in [0] + near:
            if i == 1:
                gy_copy(d).wait_recv()
            else:
                for e in range(1, n_b):
                    gb_copy(i, d, e).wait_recv()
            ga_copy(i, d).start()

    def total_phase_end(i):
        for d in range(n_c):
            ga_copy(i, d).wait_recv()

    def shifted(p):
        left, mid, right = (p[:, c * ch : (c + 1) * ch].reshape(rows, cw, ch) for c in range(3))
        pos = lax.broadcasted_iota(jnp.int32, (rows, cw, ch), 1)
        return (
            jnp.where(pos == 0, 0.0, pltpu.roll(left, 1, 1)) + mid
            + jnp.where(pos == cw - 1, 0.0, pltpu.roll(right, cw - 1, 1))
        )

    def conv_pair(k, w, t, epilogue):
        def x(j, b):
            return pads[k, t + j, pl.ds(b, rows)].reshape(rows * cw, ch)

        def taps(a, b):
            return jnp.concatenate([w[a, b, c] for c in range(3)], axis=1)

        def both(j, b):
            return jnp.concatenate([taps(j, b), taps(j - 1, b)], axis=1)

        def dot(xs, ws):
            return jnp.dot(
                jnp.concatenate(xs, axis=1), jnp.concatenate(ws, axis=0), preferred_element_type=F32
            )

        mid = [(j, b) for j in (1, 2) for b in range(3)]
        p = dot([x(j, b) for j, b in mid], [both(j, b) for j, b in mid])
        q0 = dot([x(0, b) for b in range(3)], [taps(0, b) for b in range(3)])
        q1 = dot([x(3, b) for b in range(3)], [taps(2, b) for b in range(3)])
        epilogue(t, shifted(p[:, : 3 * ch] + q0))
        epilogue(t + 1, shifted(p[:, 3 * ch :] + q1))

    inner = pl.ds(1, rows)

    def end0(t, z):
        sigma = jax.nn.sigmoid(z)
        slope1[t] = sigma * (1.0 + z * (1.0 - sigma))
        pads[1, HALO + t, inner] = (z * sigma).astype(BF16)

    def end1(t, z):
        sigma = jax.nn.sigmoid(z)
        crit_s[t] = (z * sigma).astype(BF16)
        delta = cotp[t].astype(F32) * (sigma * (1.0 + z * (1.0 - sigma)))
        pads[2, t, inner] = delta.astype(BF16)

    def end2(t, z):
        pads[3, t, inner] = (z * slope1[t]).astype(BF16)

    def end3(t, z):
        cg_s[t] = z.astype(BF16)

    def turn_weights():
        def one(i, c):
            a, b = i // 3, lax.rem(i, 3)
            for src, dst in ((w1v, w1t), (w2v, w2t)):
                for q in range(3):
                    dst[a, b, q] = src[2 - a, 2 - b, 2 - q].T
            return c
        lax.fori_loop(0, 9, one, 0)

    def turn_input(k, lo, n):
        def one(f, c):
            for r in range(rows + 2):
                xt[k, f, :, r * half : (r + 1) * half] = pads[k, f, r, pl.ds(own, half)].T
            return c
        lax.fori_loop(lo, lo + n, one, 0)

    def spread_delta(k, lo, n):
        def one(t, c):
            pos = lax.broadcasted_iota(jnp.int32, (cw, ch), 0)
            for r in range(rows):
                x = pads[k, t, r + 1].astype(F32)
                d3[t, r, :, 0:ch] = jnp.where(pos == cw - 1, 0.0, pltpu.roll(x, cw - 1, 0)).astype(BF16)
                d3[t, r, :, ch : 2 * ch] = pads[k, t, r + 1]
                d3[t, r, :, 2 * ch :] = jnp.where(pos == 0, 0.0, pltpu.roll(x, 1, 0)).astype(BF16)
            return c
        lax.fori_loop(lo, lo + n, one, 0)

    def weight_grad(k, ts, last, i):
        def one(a, c):
            z = None
            for t in ts:
                x = xt[k, t + a]
                left = jnp.concatenate([x[:, b * half : (b + rows) * half] for b in range(3)], axis=0)
                right = d3[t, :, pl.ds(own, half)].reshape(rows * half, 3 * ch)
                p = jnp.dot(left, right, preferred_element_type=F32)
                z = p if z is None else z + p
            if not last:
                acc[a] = z
            else:
                z = (z if len(ts) == frames else z + acc[a]) * grad_scale
                for b in range(3):
                    for q in range(3):
                        at = pl.multiple_of(a * (9 * ch) + (b * 3 + q) * ch, ch)
                        mine[i, pl.ds(at, ch)] = z[b * ch : (b + 1) * ch, q * ch : (q + 1) * ch].astype(BF16)
            return c
        for a in range(3):
            one(a, 0)

    for t in range(step):
        loads[2 * t].wait()
    for t in (1, 0):
        cross_copy(0, t).start()
    for t in range(step):
        loads[2 * t + 1].wait()

    def publish_clip(who, fs):
        @pl.when(who)
        def _():
            for f in fs:
                if f >= frames:
                    send_frame(0, f - frames)
                send_rows(0, f)

    publish_clip(second, (frames + 1, frames))
    publish_clip(first, (HALO + 1, HALO))
    for t in (1, 0):
        cross_copy(1, t).start()
    loads[2 * step].wait()
    loads[2 * step + 1].wait()
    turn_weights()
    for t in (1, 0):
        cross_copy(0, t).wait_recv()
        publish_clip(first, (HALO + step + t,))
        publish_clip(second, (HALO + t,))

    local_f = tuple(range(HALO, HALO + frames))
    local_b = tuple(range(frames))

    wait_rows(0, local_f)
    conv_pair(0, w1v, 2, end0)
    for t in (1, 0):
        send_frame(1, t)
        send_rows(1, frames + t)
    pass_halo(0, 1)
    pass_halo(0, 0)
    wait_halo(0)
    conv_pair(0, w1v, 0, end0)
    for f in (HALO + 1, HALO):
        send_rows(1, f)
    turn_input(0, 0, frames + HALO)

    for t in range(step):
        loads[2 * step + 2 + t].wait()
        cross_copy(1, t).wait_recv()
    wait_rows(1, local_f)
    pass_halo(1, 1)
    conv_pair(1, w2v, 2, end1)
    for t in (2, 3):
        send_rows(2, t)

    def send_out(i, who):
        @pl.when(who)
        def _():
            for t in range(step):
                out_copy(i, t).start()

    send_out(0, first)
    pass_halo(1, 0)
    turn_input(1, HALO, frames)
    spread_delta(2, 2, 2)
    wait_halo(1)
    conv_pair(1, w2v, 0, end1)
    for t in (0, 1):
        send_frame(2, t)
        send_rows(2, t)
    keep(0)
    turn_input(1, 0, HALO)
    spread_delta(2, 0, 2)
    weight_grad(1, local_b, True, 1)
    sum_phase_a(1)

    wait_rows(2, local_b)
    conv_pair(2, w2t, 0, end2)
    for t in (0, 1):
        send_frame(3, t)
        send_rows(3, t)
    sum_phase_b(1)
    send_out(0, second)
    pass_halo(2, 0)
    spread_delta(3, 0, 2)
    weight_grad(0, (0, 1), False, 0)
    pass_halo(2, 1)
    wait_halo(2)
    conv_pair(2, w2t, 2, end2)
    for t in (2, 3):
        send_rows(3, t)
    sum_phase_c(1, order)
    spread_delta(3, 2, 2)
    weight_grad(0, (2, 3), True, 0)
    sum_phase_a(0)

    pass_halo(3, 0)
    pass_halo(3, 1)
    wait_rows(3, local_b)
    conv_pair(3, w1t, 0, end3)
    sum_phase_b(0)
    total_phase_z(1)
    wait_halo(3)
    conv_pair(3, w1t, 2, end3)
    keep(1)
    sum_phase_c(0, order[:1])
    total_phase_x()
    send_out(1, second)
    send_out(1, first)
    sum_phase_c(0, order[1:])
    total_phase_y([0] + near[:1])
    total_phase_z(0)
    total_phase_y(near[1:])
    total_phase_b(0)
    total_phase_a(1)
    total_phase_a(0)
    total_phase_end(1)
    total_phase_end(0)

    for i in range(2):
        for t in range(step):
            cross_copy(i, t).wait_send()
            out_copy(i, t).wait()
        a_copy(i).wait_send()
        for d in range(n_c):
            ga_copy(i, d).wait_send()
            for e in range(1, n_b):
                b_copy(i, d, e).wait_send()
            if i == 1:
                gx_copy(d).wait_send()
                gy_copy(d).wait_send()
            else:
                for e in range(1, n_b):
                    gb_copy(i, d, e).wait_send()
        for d in range(1, n_c):
            z_copy(i, d).wait_send()
            gz_copy(i, d).wait_send()
    for k in range(4):
        fwd = k < 2

        @pl.when(later if fwd else earlier)
        def _():
            for t in range(HALO):
                frame_copy(k, t).wait_send()

        @pl.when(jnp.logical_and(later if fwd else earlier, facing))
        def _():
            for t in range(HALO):
                corner_copy(k, t).wait_send()

        @pl.when(earlier if fwd else later)
        def _():
            for t in range(HALO):
                mate_copy(k, t).wait_send()
        for f in local_f if fwd else local_b:
            for way, there in ((0, below), (1, above)):
                @pl.when(there)
                def _():
                    row_copy(k, f, way).wait_send()


def finish(t1, t2, critic, clip_grad, g1, g2, critic_out, clip_grad_out, wide, g_sem, o_sem):
    copies = [
        pltpu.make_async_copy(src, dst, o_sem.at[i])
        for i, (src, dst) in enumerate(((critic, critic_out), (clip_grad, clip_grad_out)))
    ]
    for copy in copies:
        copy.start()
    part = wide.shape[1] // 3
    for i, (src, dst) in enumerate(((t1, g1), (t2, g2))):
        for a in range(3):
            at = pl.ds(a * part, part)
            wide[i, at] = src[at].astype(F32)
            copy = pltpu.make_async_copy(wide.at[i, at], dst.at[at], g_sem.at[i, a])
            copy.start()
            copies.append(copy)
    for copy in copies:
        copy.wait()


def on_device(n_frame, n_row, clip, first_kernel, second_kernel, cotangent):
    step, rows, width, ch = clip.shape
    grad_scale = 1.0 / float(step * n_frame * rows * n_row * width) ** 0.5
    n = n_frame * n_row
    frames, cw = 2 * step, width // 2 + MARGIN
    vmem, hbm = pl.BlockSpec(memory_space=pltpu.VMEM), pl.BlockSpec(memory_space=pltpu.HBM)
    weights = first_kernel.shape
    length = 27 * ch
    padded = -(-length // (16 * n)) * 16 * n
    counts = (2, n_row // 2 * 2, n_frame // 2)
    size_a = padded // counts[0]
    piece = size_a // (counts[1] * counts[2])
    sems = pltpu.SemaphoreType.DMA
    block = (frames, rows, cw, ch)
    critic, clip_grad, t1, t2 = pl.pallas_call(
        functools.partial(kernel, n_frame, n_row, grad_scale),
        out_shape=(
            jax.ShapeDtypeStruct(clip.shape, BF16),
            jax.ShapeDtypeStruct(clip.shape, BF16),
            jax.ShapeDtypeStruct((padded, ch), BF16),
            jax.ShapeDtypeStruct((padded, ch), BF16),
        ),
        in_specs=[hbm] * 4,
        out_specs=(vmem,) * 4,
        scratch_shapes=[
            pltpu.VMEM((4, frames + HALO, rows + 2, cw, ch), BF16),
            pltpu.VMEM((step, rows, cw, ch), BF16),
            pltpu.VMEM(block, BF16),
            pltpu.VMEM(block, BF16),
            pltpu.VMEM(block, BF16),
            pltpu.VMEM(block, F32),
            pltpu.VMEM(weights, BF16),
            pltpu.VMEM(weights, BF16),
            pltpu.VMEM(weights, BF16),
            pltpu.VMEM(weights, BF16),
            pltpu.VMEM((2, frames + HALO, ch, (rows + 2) * (width // 2)), BF16),
            pltpu.VMEM((frames, rows, cw, 3 * ch), BF16),
            pltpu.VMEM((3, 3 * ch, 3 * ch), F32),
            pltpu.VMEM((2, padded, ch), BF16),
            pltpu.VMEM((2, size_a, ch), BF16),
            pltpu.VMEM((2, size_a, ch), BF16),
            pltpu.VMEM((2, counts[2], counts[1] - 1, piece, ch), BF16),
            pltpu.VMEM((2, counts[2] - 1, piece, ch), BF16),
            pltpu.VMEM((2, counts[2] - 1, piece, ch), BF16),
            sems((3 * step + 2,)),
            sems((2, step)), sems((2, step)),
            sems((2, step)), sems((2, step)),
            sems((4, HALO)), sems((4, HALO)),
            sems((4, HALO)), sems((4, HALO)),
            sems((4, frames + HALO, 2)), sems((4, frames + HALO, 2)),
            sems((2,)), sems((2,)),
            sems((2, counts[2], counts[1] - 1)), sems((2, counts[2], counts[1] - 1)),
            sems((2, counts[2] - 1)), sems((2, counts[2] - 1)),
            sems((2, counts[2])), sems((2, counts[2])),
            sems((2, counts[2], counts[1] - 1)), sems((2, counts[2], counts[1] - 1)),
            sems((2, counts[2] - 1)), sems((2, counts[2] - 1)),
        ],
        compiler_params=pltpu.CompilerParams(
            collective_id=0, has_side_effects=True, vmem_limit_bytes=32 * 2**20
        ),
    )(*(pltpu.with_memory_space_constraint(v, pltpu.HBM) for v in (clip, first_kernel, second_kernel, cotangent)))
    flat = jax.ShapeDtypeStruct((length, ch), F32)
    g1, g2, critic, clip_grad = pl.pallas_call(
        finish,
        out_shape=(flat, flat, jax.ShapeDtypeStruct(clip.shape, BF16), jax.ShapeDtypeStruct(clip.shape, BF16)),
        in_specs=[vmem] * 4,
        out_specs=(hbm,) * 4,
        scratch_shapes=[pltpu.VMEM((2, length, ch), F32), sems((2, 3)), sems((2,))],
        compiler_params=pltpu.CompilerParams(vmem_limit_bytes=16 * 2**20),
    )(t1, t2, critic, clip_grad)
    return critic, clip_grad, g1.reshape(weights), g2.reshape(weights)


def solution(mesh):
    placed = (P("frame", "row", None, None), P(), P(), P("frame", "row", None, None))
    return jax.shard_map(
        functools.partial(on_device, mesh.shape["frame"], mesh.shape["row"]),
        mesh=mesh,
        in_specs=placed,
        out_specs=(P("frame", "row", None, None), P("frame", "row", None, None), P(), P()),
        check_vma=False,
    )
```

```python
import functools

import jax
import jax.numpy as jnp
from jax import lax
from jax.experimental import pallas as pl
from jax.experimental.pallas import tpu as pltpu
from jax.sharding import PartitionSpec as P

MESH = pl.DeviceIdType.MESH
BF16, F32 = jnp.bfloat16, jnp.float32
MARGIN = 8
HALO = 2


def sum_groups(n_frame, n_row, me_f, me_r):
    pair, member = me_f // 2, lax.rem(me_f, 2)
    side, core = me_r // 2, lax.rem(me_r, 2)
    return (
        (2, core, lambda j: {"row": side * 2 + j}),
        (n_row // 2 * 2, side * 2 + member, lambda j: {"row": j // 2 * 2 + core, "frame": pair * 2 + lax.rem(j, 2)}),
        (n_frame // 2, pair, lambda j: {"frame": j * 2 + member}),
    )


def kernel(
    n_frame, n_row, grad_scale,
    clip, w1, w2, cot,
    critic, clip_grad, total1, total2,
    pads, cross, cotp, crit_s, cg_s, slope1, w1v, w2v, w1t, w2t, xt, d3, acc,
    mine, land_a, sum_a, land_b, sum_b, land_c,
    l_sem, x_send, x_recv, o_send, o_recv, f_send, f_recv, c_send, c_recv, r_send, r_recv,
    a_send, a_recv, b_send, b_recv, z_send, z_recv, ga_send, ga_recv, gb_send, gb_recv, gz_send, gz_recv,
):
    step, rows, width, ch = clip.shape
    half = width // 2
    cw = half + MARGIN
    frames = 2 * step
    me_f, me_r = lax.axis_index("frame"), lax.axis_index("row")
    member = lax.rem(me_f, 2)
    first, second = member == 0, member == 1
    later, earlier = me_f < n_frame - 2, me_f > 1
    below, above = me_r < n_row - 1, me_r > 0
    partner = {"frame": me_f + 1 - 2 * member}
    groups = sum_groups(n_frame, n_row, me_f, me_r)
    own = pl.multiple_of(member * MARGIN, MARGIN)
    odd = lax.rem(me_r, 2)
    facing = jnp.logical_or(jnp.logical_and(odd == 1, below), jnp.logical_and(odd == 0, above))
    mate, across = me_r + 1 - 2 * odd, me_r - 1 + 2 * odd

    def start_of(who):
        return pl.multiple_of(who * (half - MARGIN), MARGIN)

    barrier = pltpu.get_barrier_semaphore()
    for there, who in ((below, {"row": me_r + 1}), (above, {"row": me_r - 1})):
        @pl.when(there)
        def _():
            pl.semaphore_signal(barrier, inc=1, device_id=who, device_id_type=MESH)
    greeted = below.astype(jnp.int32) + above.astype(jnp.int32)
    for there, way in ((later, 2), (earlier, -2)):
        met = jnp.logical_and(there, facing)

        @pl.when(met)
        def _():
            who = {"frame": me_f + way, "row": across}
            pl.semaphore_signal(barrier, inc=1, device_id=who, device_id_type=MESH)
        greeted = greeted + met.astype(jnp.int32)
    for count, index, device in groups[1:]:
        for d in range(1, count):
            pl.semaphore_signal(barrier, inc=1, device_id=device(lax.rem(index + d, count)), device_id_type=MESH)
        greeted = greeted + (count - 1)

    loads = []
    for t in range(step):
        mine_at, other_at = pl.ds(start_of(member), cw), pl.ds(start_of(1 - member), cw)
        loads.append((clip.at[t, :, other_at], cross.at[t]))
        loads.append((clip.at[t, :, mine_at], pads.at[0, HALO + step * member + t, pl.ds(1, rows)]))
    loads.append((w1, w1v))
    loads.append((w2, w2v))
    for t in range(step):
        loads.append((cot.at[t, :, mine_at], cotp.at[step * member + t]))
    loads = [pltpu.make_async_copy(a, b, l_sem.at[i]) for i, (a, b) in enumerate(loads)]
    for load in loads:
        load.start()

    def zero(ref):
        ref[...] = jnp.zeros(ref.shape, ref.dtype)

    for k in range(4):
        @pl.when(jnp.logical_not(earlier if k < 2 else later))
        def _():
            for f in ((0, 1) if k < 2 else (frames, frames + 1)):
                zero(pads.at[k, f])

        @pl.when(jnp.logical_not(above))
        def _():
            for f in range(frames + HALO):
                zero(pads.at[k, f, 0])

        @pl.when(jnp.logical_not(below))
        def _():
            for f in range(frames + HALO):
                zero(pads.at[k, f, rows + 1])
    used = 27 * ch
    for i in range(2):
        mine[i, pl.ds(used, mine.shape[1] - used)] = jnp.zeros((mine.shape[1] - used, ch), BF16)

    pl.semaphore_wait(barrier, greeted)

    def remote(src, dst, send, recv, who):
        return pltpu.make_async_remote_copy(
            src_ref=src, dst_ref=dst, send_sem=send, recv_sem=recv, device_id=who, device_id_type=MESH
        )

    def cross_copy(i, t):
        if i == 0:
            src, dst = cross.at[t], pads.at[0, HALO + step * member + t, pl.ds(1, rows)]
        else:
            src, dst = cot.at[t, :, pl.ds(start_of(1 - member), cw)], cotp.at[step * member + t]
        return remote(src, dst, x_send.at[i, t], x_recv.at[i, t], partner)

    def out_copy(i, t):
        src, dst = ((crit_s, critic), (cg_s, clip_grad))[i]
        return remote(
            src.at[step * (1 - member) + t, :, pl.ds(own, half)],
            dst.at[t, :, pl.ds(pl.multiple_of(member * half, half), half)],
            o_send.at[i, t], o_recv.at[i, t], partner,
        )

    def keep(i):
        src, dst = ((crit_s, critic), (cg_s, clip_grad))[i]
        for t in range(step):
            dst[t, :, pl.ds(pl.multiple_of(member * half, half), half)] = src[step * member + t, :, pl.ds(own, half)]

    def frame_copy(k, t, part):
        fwd = k < 2
        src, dst = (frames + t, t) if fwd else (t, frames + t)
        at = (pl.ds(rows - odd * (rows - 1), 1), pl.ds(1 + odd, rows - 1))[part]
        return remote(
            pads.at[k, src, at], pads.at[k, dst, at],
            f_send.at[k, t, part], f_recv.at[k, t, part], {"frame": me_f + 2 if fwd else me_f - 2},
        )

    def row_copy(k, f, way):
        src, dst = ((rows, 0), (1, rows + 1))[way]
        return remote(
            pads.at[k, f, src], pads.at[k, f, dst],
            r_send.at[k, f, way], r_recv.at[k, f, way], {"row": me_r + 1 if way == 0 else me_r - 1},
        )

    def send_rows(k, f):
        @pl.when(below)
        def _():
            row_copy(k, f, 0).start()

        @pl.when(above)
        def _():
            row_copy(k, f, 1).start()

    def wait_rows(k, fs):
        for f in fs:
            @pl.when(above)
            def _():
                row_copy(k, f, 0).wait_recv()

            @pl.when(below)
            def _():
                row_copy(k, f, 1).wait_recv()

    def corner_copy(k, t):
        fwd = k < 2
        src, dst = (frames + t, t) if fwd else (t, frames + t)
        return remote(
            pads.at[k, src, 1 + odd * (rows - 1)], pads.at[k, dst, (1 - odd) * (rows + 1)],
            c_send.at[k, t], c_recv.at[k, t], {"frame": me_f + 2 if fwd else me_f - 2, "row": across},
        )

    def mate_copy(k, t):
        f = t if k < 2 else frames + t
        return remote(
            pads.at[k, f, rows - odd * (rows - 1)], pads.at[k, f, odd * (rows + 1)],
            r_send.at[k, f, 0], r_recv.at[k, f, 0], {"row": mate},
        )

    def send_frames(k, ts):
        there = later if k < 2 else earlier
        for t in ts:
            @pl.when(there)
            def _():
                frame_copy(k, t, 0).start()
        for t in ts:
            @pl.when(there)
            def _():
                frame_copy(k, t, 1).start()

            @pl.when(jnp.logical_and(there, facing))
            def _():
                corner_copy(k, t).start()

    def pass_halo(k, t):
        @pl.when(earlier if k < 2 else later)
        def _():
            frame_copy(k, t, 0).wait_recv()
            mate_copy(k, t).start()

    def wait_halo(k):
        there = earlier if k < 2 else later

        @pl.when(there)
        def _():
            for t in range(HALO):
                frame_copy(k, t, 1).wait_recv()
                mate_copy(k, t).wait_recv()

        @pl.when(jnp.logical_and(there, facing))
        def _():
            for t in range(HALO):
                corner_copy(k, t).wait_recv()

    (_, core, to_core), (n_b, in_b, to_b), (n_c, in_c, to_c) = groups
    half_rows = sum_a.shape[1]
    piece = half_rows // (n_b * n_c)

    def aligned(x):
        return pl.multiple_of(x, 16)

    def block(q):
        return aligned(q * (n_b * piece))

    def a_copy(i):
        src = mine.at[i, pl.ds(aligned((1 - core) * half_rows), half_rows)]
        return remote(src, land_a.at[i], a_send.at[i], a_recv.at[i], to_core(1 - core))

    def b_copy(i, d, e):
        peer = lax.rem(in_b + e, n_b)
        src = sum_a.at[i, pl.ds(aligned(block(lax.rem(in_c + d, n_c)) + peer * piece), piece)]
        return remote(src, land_b.at[i, d, e - 1], b_send.at[i, d, e - 1], b_recv.at[i, d, e - 1], to_b(peer))

    def z_copy(i, d):
        peer = lax.rem(in_c + d, n_c)
        return remote(sum_b.at[i, d - 1], land_c.at[i, d - 1], z_send.at[i, d - 1], z_recv.at[i, d - 1], to_c(peer))

    near = sorted(range(1, n_c), key=lambda d: min(d, n_c - d))
    order = tuple(reversed(near))

    def sum_phase_a(i):
        a_copy(i).start()

    def sum_phase_b(i):
        a_copy(i).wait_recv()
        kept = mine[i, pl.ds(aligned(core * half_rows), half_rows)].astype(F32)
        sum_a[i] = (kept + land_a[i].astype(F32)).astype(BF16)
        for d in order + (0,):
            for e in range(1, n_b):
                b_copy(i, d, e).start()

    def plane_sum(i, d):
        for e in range(1, n_b):
            b_copy(i, d, e).wait_recv()
        z = sum_a[i, pl.ds(aligned(block(lax.rem(in_c + d, n_c)) + in_b * piece), piece)].astype(F32)
        for e in range(1, n_b):
            z = z + land_b[i, d, e - 1].astype(F32)
        return z

    def sum_phase_c(i, ds):
        for d in ds:
            sum_b[i, d - 1] = plane_sum(i, d).astype(BF16)
            z_copy(i, d).start()

    def total_at(i, q, j, n):
        lo = aligned(core * half_rows + block(q) + j * piece)
        return (total1, total2)[i].at[pl.ds(lo, n)]

    def gz_copy(i, d):
        part = total_at(i, in_c, in_b, piece)
        return remote(part, part, gz_send.at[i, d - 1], gz_recv.at[i, d - 1], to_c(lax.rem(in_c + d, n_c)))

    def source(d):
        return lax.rem(in_c + n_c - d, n_c)

    def gb_copy(i, d, e):
        part = total_at(i, source(d), in_b, piece)
        return remote(
            part, part, gb_send.at[i, d, e - 1], gb_recv.at[i, d, e - 1], to_b(lax.rem(in_b + e, n_b))
        )

    def ga_copy(i, d):
        part = total_at(i, source(d), 0, n_b * piece)
        return remote(part, part, ga_send.at[i, d], ga_recv.at[i, d], to_core(1 - core))

    def gx_copy(d):
        part = total_at(1, source(d), in_b, piece)
        return remote(part, part, gb_send.at[1, d, 0], gb_recv.at[1, d, 0], partner)

    def gy_copy(d):
        side = me_r // 2
        part = total_at(1, source(d), side * 2, 2 * piece)
        return remote(part, part, gb_send.at[1, d, 1], gb_recv.at[1, d, 1], {"row": me_r + 2 - 4 * side})

    def total_phase_x():
        for d in near:
            gz_copy(1, d).wait_recv()
            gx_copy(d).start()

    def total_phase_y(ds):
        for d in ds:
            gx_copy(d).wait_recv()
            gy_copy(d).start()

    def total_phase_z(i):
        z = plane_sum(i, 0)
        for d in range(1, n_c):
            z_copy(i, d).wait_recv()
            z = z + land_c[i, d - 1].astype(F32)
        total_at(i, in_c, in_b, piece)[...] = z.astype(BF16)
        for d in order:
            gz_copy(i, d).start()
        if i == 1:
            gx_copy(0).start()
        else:
            for e in range(1, n_b):
                gb_copy(i, 0, e).start()

    def total_phase_b(i):
        for d in near:
            gz_copy(i, d).wait_recv()
            for e in range(1, n_b):
                gb_copy(i, d, e).start()

    def total_phase_a(i):
        for d in [0] + near:
            if i == 1:
                gy_copy(d).wait_recv()
            else:
                for e in range(1, n_b):
                    gb_copy(i, d, e).wait_recv()
            ga_copy(i, d).start()

    def total_phase_end(i):
        for d in range(n_c):
            ga_copy(i, d).wait_recv()

    def shifted(p):
        left, mid, right = (p[:, c * ch : (c + 1) * ch].reshape(rows, cw, ch) for c in range(3))
        pos = lax.broadcasted_iota(jnp.int32, (rows, cw, ch), 1)
        return (
            jnp.where(pos == 0, 0.0, pltpu.roll(left, 1, 1)) + mid
            + jnp.where(pos == cw - 1, 0.0, pltpu.roll(right, cw - 1, 1))
        )

    def conv_pair(k, w, t, epilogue):
        def x(j, b):
            return pads[k, t + j, pl.ds(b, rows)].reshape(rows * cw, ch)

        def taps(a, b):
            return jnp.concatenate([w[a, b, c] for c in range(3)], axis=1)

        def both(j, b):
            return jnp.concatenate([taps(j, b), taps(j - 1, b)], axis=1)

        def dot(xs, ws):
            return jnp.dot(
                jnp.concatenate(xs, axis=1), jnp.concatenate(ws, axis=0), preferred_element_type=F32
            )

        mid = [(j, b) for j in (1, 2) for b in range(3)]
        p = dot([x(j, b) for j, b in mid], [both(j, b) for j, b in mid])
        q0 = dot([x(0, b) for b in range(3)], [taps(0, b) for b in range(3)])
        q1 = dot([x(3, b) for b in range(3)], [taps(2, b) for b in range(3)])
        epilogue(t, shifted(p[:, : 3 * ch] + q0))
        epilogue(t + 1, shifted(p[:, 3 * ch :] + q1))

    inner = pl.ds(1, rows)

    def end0(t, z):
        sigma = jax.nn.sigmoid(z)
        slope1[t] = sigma * (1.0 + z * (1.0 - sigma))
        pads[1, HALO + t, inner] = (z * sigma).astype(BF16)

    def end1(t, z):
        sigma = jax.nn.sigmoid(z)
        crit_s[t] = (z * sigma).astype(BF16)
        delta = cotp[t].astype(F32) * (sigma * (1.0 + z * (1.0 - sigma)))
        pads[2, t, inner] = delta.astype(BF16)

    def end2(t, z):
        pads[3, t, inner] = (z * slope1[t]).astype(BF16)

    def end3(t, z):
        cg_s[t] = z.astype(BF16)

    def turn_weights():
        def one(i, c):
            a, b = i // 3, lax.rem(i, 3)
            for src, dst in ((w1v, w1t), (w2v, w2t)):
                for q in range(3):
                    dst[a, b, q] = src[2 - a, 2 - b, 2 - q].T
            return c
        lax.fori_loop(0, 9, one, 0)

    def turn_input(k, lo, n):
        def one(f, c):
            for r in range(rows + 2):
                xt[k, f, :, r * half : (r + 1) * half] = pads[k, f, r, pl.ds(own, half)].T
            return c
        lax.fori_loop(lo, lo + n, one, 0)

    def spread_delta(k, lo, n):
        def one(t, c):
            pos = lax.broadcasted_iota(jnp.int32, (cw, ch), 0)
            for r in range(rows):
                x = pads[k, t, r + 1].astype(F32)
                d3[t, r, :, 0:ch] = jnp.where(pos == cw - 1, 0.0, pltpu.roll(x, cw - 1, 0)).astype(BF16)
                d3[t, r, :, ch : 2 * ch] = pads[k, t, r + 1]
                d3[t, r, :, 2 * ch :] = jnp.where(pos == 0, 0.0, pltpu.roll(x, 1, 0)).astype(BF16)
            return c
        lax.fori_loop(lo, lo + n, one, 0)

    def weight_grad(k, ts, last, i):
        def one(a, c):
            z = None
            for t in ts:
                x = xt[k, t + a]
                left = jnp.concatenate([x[:, b * half : (b + rows) * half] for b in range(3)], axis=0)
                right = d3[t, :, pl.ds(own, half)].reshape(rows * half, 3 * ch)
                p = jnp.dot(left, right, preferred_element_type=F32)
                z = p if z is None else z + p
            if not last:
                acc[a] = z
            else:
                z = (z if len(ts) == frames else z + acc[a]) * grad_scale
                for b in range(3):
                    for q in range(3):
                        at = pl.multiple_of(a * (9 * ch) + (b * 3 + q) * ch, ch)
                        mine[i, pl.ds(at, ch)] = z[b * ch : (b + 1) * ch, q * ch : (q + 1) * ch].astype(BF16)
            return c
        for a in range(3):
            one(a, 0)

    for t in range(step):
        loads[2 * t].wait()
    for t in (1, 0):
        cross_copy(0, t).start()
    for t in range(step):
        loads[2 * t + 1].wait()

    def publish_clip(who, fs):
        @pl.when(who)
        def _():
            if fs[0] >= frames:
                send_frames(0, [f - frames for f in fs])
            for f in fs:
                send_rows(0, f)

    publish_clip(second, (frames + 1, frames))
    publish_clip(first, (HALO + 1, HALO))
    for t in (1, 0):
        cross_copy(1, t).start()
    loads[2 * step].wait()
    loads[2 * step + 1].wait()
    turn_weights()
    for t in (1, 0):
        cross_copy(0, t).wait_recv()
        publish_clip(first, (HALO + step + t,))
        publish_clip(second, (HALO + t,))

    local_f = tuple(range(HALO, HALO + frames))
    local_b = tuple(range(frames))

    wait_rows(0, local_f)
    conv_pair(0, w1v, 2, end0)
    for t in (1, 0):
        send_rows(1, frames + t)
    send_frames(1, (1, 0))
    pass_halo(0, 1)
    pass_halo(0, 0)
    wait_halo(0)
    conv_pair(0, w1v, 0, end0)
    for f in (HALO + 1, HALO):
        send_rows(1, f)
    turn_input(0, 0, frames + HALO)

    for t in range(step):
        loads[2 * step + 2 + t].wait()
        cross_copy(1, t).wait_recv()
    wait_rows(1, local_f)
    pass_halo(1, 1)
    pass_halo(1, 0)
    conv_pair(1, w2v, 2, end1)
    for t in (2, 3):
        send_rows(2, t)

    def send_out(i, who):
        @pl.when(who)
        def _():
            for t in range(step):
                out_copy(i, t).start()

    send_out(0, first)
    turn_input(1, HALO, frames)
    spread_delta(2, 2, 2)
    wait_halo(1)
    conv_pair(1, w2v, 0, end1)
    for t in (0, 1):
        send_rows(2, t)
    send_frames(2, (0, 1))
    keep(0)
    turn_input(1, 0, HALO)
    spread_delta(2, 0, 2)
    weight_grad(1, local_b, True, 1)
    sum_phase_a(1)

    wait_rows(2, local_b)
    conv_pair(2, w2t, 0, end2)
    for t in (0, 1):
        send_rows(3, t)
    send_frames(3, (0, 1))
    sum_phase_b(1)
    send_out(0, second)
    pass_halo(2, 0)
    spread_delta(3, 0, 2)
    pass_halo(2, 1)
    weight_grad(0, (0, 1), False, 0)
    wait_halo(2)
    conv_pair(2, w2t, 2, end2)
    for t in (2, 3):
        send_rows(3, t)
    spread_delta(3, 2, 2)
    sum_phase_c(1, order[:2])
    weight_grad(0, (2, 3), True, 0)
    sum_phase_a(0)
    sum_phase_c(1, order[2:])

    pass_halo(3, 0)
    pass_halo(3, 1)
    wait_rows(3, local_b)
    conv_pair(3, w1t, 0, end3)
    sum_phase_b(0)
    total_phase_z(1)
    wait_halo(3)
    conv_pair(3, w1t, 2, end3)
    keep(1)
    sum_phase_c(0, order[:1])
    total_phase_x()
    send_out(1, second)
    send_out(1, first)
    sum_phase_c(0, order[1:])
    total_phase_y([0] + near[:1])
    total_phase_z(0)
    total_phase_y(near[1:])
    total_phase_b(0)
    total_phase_a(1)
    total_phase_a(0)
    total_phase_end(1)
    total_phase_end(0)

    for i in range(2):
        for t in range(step):
            cross_copy(i, t).wait_send()
            out_copy(i, t).wait()
        a_copy(i).wait_send()
        for d in range(n_c):
            ga_copy(i, d).wait_send()
            for e in range(1, n_b):
                b_copy(i, d, e).wait_send()
            if i == 1:
                gx_copy(d).wait_send()
                gy_copy(d).wait_send()
            else:
                for e in range(1, n_b):
                    gb_copy(i, d, e).wait_send()
        for d in range(1, n_c):
            z_copy(i, d).wait_send()
            gz_copy(i, d).wait_send()
    for k in range(4):
        fwd = k < 2

        @pl.when(later if fwd else earlier)
        def _():
            for t in range(HALO):
                for part in range(2):
                    frame_copy(k, t, part).wait_send()

        @pl.when(jnp.logical_and(later if fwd else earlier, facing))
        def _():
            for t in range(HALO):
                corner_copy(k, t).wait_send()

        @pl.when(earlier if fwd else later)
        def _():
            for t in range(HALO):
                mate_copy(k, t).wait_send()
        for f in local_f if fwd else local_b:
            for way, there in ((0, below), (1, above)):
                @pl.when(there)
                def _():
                    row_copy(k, f, way).wait_send()


def finish(t1, t2, critic, clip_grad, g1, g2, critic_out, clip_grad_out, wide, g_sem, o_sem):
    copies = [
        pltpu.make_async_copy(src, dst, o_sem.at[i])
        for i, (src, dst) in enumerate(((critic, critic_out), (clip_grad, clip_grad_out)))
    ]
    for copy in copies:
        copy.start()
    part = wide.shape[1] // 3
    for i, (src, dst) in enumerate(((t1, g1), (t2, g2))):
        for a in range(3):
            at = pl.ds(a * part, part)
            wide[i, at] = src[at].astype(F32)
            copy = pltpu.make_async_copy(wide.at[i, at], dst.at[at], g_sem.at[i, a])
            copy.start()
            copies.append(copy)
    for copy in copies:
        copy.wait()


def on_device(n_frame, n_row, clip, first_kernel, second_kernel, cotangent):
    step, rows, width, ch = clip.shape
    grad_scale = 1.0 / float(step * n_frame * rows * n_row * width) ** 0.5
    n = n_frame * n_row
    frames, cw = 2 * step, width // 2 + MARGIN
    vmem, hbm = pl.BlockSpec(memory_space=pltpu.VMEM), pl.BlockSpec(memory_space=pltpu.HBM)
    weights = first_kernel.shape
    length = 27 * ch
    padded = -(-length // (16 * n)) * 16 * n
    counts = (2, n_row // 2 * 2, n_frame // 2)
    size_a = padded // counts[0]
    piece = size_a // (counts[1] * counts[2])
    sems = pltpu.SemaphoreType.DMA
    block = (frames, rows, cw, ch)
    critic, clip_grad, t1, t2 = pl.pallas_call(
        functools.partial(kernel, n_frame, n_row, grad_scale),
        out_shape=(
            jax.ShapeDtypeStruct(clip.shape, BF16),
            jax.ShapeDtypeStruct(clip.shape, BF16),
            jax.ShapeDtypeStruct((padded, ch), BF16),
            jax.ShapeDtypeStruct((padded, ch), BF16),
        ),
        in_specs=[hbm] * 4,
        out_specs=(vmem,) * 4,
        scratch_shapes=[
            pltpu.VMEM((4, frames + HALO, rows + 2, cw, ch), BF16),
            pltpu.VMEM((step, rows, cw, ch), BF16),
            pltpu.VMEM(block, BF16),
            pltpu.VMEM(block, BF16),
            pltpu.VMEM(block, BF16),
            pltpu.VMEM(block, F32),
            pltpu.VMEM(weights, BF16),
            pltpu.VMEM(weights, BF16),
            pltpu.VMEM(weights, BF16),
            pltpu.VMEM(weights, BF16),
            pltpu.VMEM((2, frames + HALO, ch, (rows + 2) * (width // 2)), BF16),
            pltpu.VMEM((frames, rows, cw, 3 * ch), BF16),
            pltpu.VMEM((3, 3 * ch, 3 * ch), F32),
            pltpu.VMEM((2, padded, ch), BF16),
            pltpu.VMEM((2, size_a, ch), BF16),
            pltpu.VMEM((2, size_a, ch), BF16),
            pltpu.VMEM((2, counts[2], counts[1] - 1, piece, ch), BF16),
            pltpu.VMEM((2, counts[2] - 1, piece, ch), BF16),
            pltpu.VMEM((2, counts[2] - 1, piece, ch), BF16),
            sems((3 * step + 2,)),
            sems((2, step)), sems((2, step)),
            sems((2, step)), sems((2, step)),
            sems((4, HALO, 2)), sems((4, HALO, 2)),
            sems((4, HALO)), sems((4, HALO)),
            sems((4, frames + HALO, 2)), sems((4, frames + HALO, 2)),
            sems((2,)), sems((2,)),
            sems((2, counts[2], counts[1] - 1)), sems((2, counts[2], counts[1] - 1)),
            sems((2, counts[2] - 1)), sems((2, counts[2] - 1)),
            sems((2, counts[2])), sems((2, counts[2])),
            sems((2, counts[2], counts[1] - 1)), sems((2, counts[2], counts[1] - 1)),
            sems((2, counts[2] - 1)), sems((2, counts[2] - 1)),
        ],
        compiler_params=pltpu.CompilerParams(
            collective_id=0, has_side_effects=True, vmem_limit_bytes=32 * 2**20
        ),
    )(*(pltpu.with_memory_space_constraint(v, pltpu.HBM) for v in (clip, first_kernel, second_kernel, cotangent)))
    flat = jax.ShapeDtypeStruct((length, ch), F32)
    g1, g2, critic, clip_grad = pl.pallas_call(
        finish,
        out_shape=(flat, flat, jax.ShapeDtypeStruct(clip.shape, BF16), jax.ShapeDtypeStruct(clip.shape, BF16)),
        in_specs=[vmem] * 4,
        out_specs=(hbm,) * 4,
        scratch_shapes=[pltpu.VMEM((2, length, ch), F32), sems((2, 3)), sems((2,))],
        compiler_params=pltpu.CompilerParams(vmem_limit_bytes=16 * 2**20),
    )(t1, t2, critic, clip_grad)
    return critic, clip_grad, g1.reshape(weights), g2.reshape(weights)


def solution(mesh):
    placed = (P("frame", "row", None, None), P(), P(), P("frame", "row", None, None))
    return jax.shard_map(
        functools.partial(on_device, mesh.shape["frame"], mesh.shape["row"]),
        mesh=mesh,
        in_specs=placed,
        out_specs=(P("frame", "row", None, None), P("frame", "row", None, None), P(), P()),
        check_vma=False,
    )
```
